32 devices in a mesh: space: 16 (over z, y, core), tensor: 2 (over x).
Axes of the slice: x: 2, y: 2, z: 4, core: 2. Of those that a mesh axis runs over, the one named last changes fastest.
Arguments:
- tokens: bfloat16 [14336, 1024], P('space', 'tensor'), may hold values from -6 to 6
- first_weight: bfloat16 [1024, 1024], P(None, 'tensor'), may hold values from -0.1875 to 0.1875
- second_weight: bfloat16 [1024, 1024], P(None, 'tensor'), may hold values from -0.1875 to 0.1875
- head_weight: bfloat16 [352, 1024], P('tensor'), may hold values from -0.1875 to 0.1875
- targets: float32 [352, 14336], P('tensor', 'space'), may hold values from -6 to 6
- land_mask: int32 [4, 14336], P(None, 'space'), may hold values from 0 to 1, as said below
- variable_kind: int32 [88], P('tensor'), may hold values from 0 to 2
- loss_scale: float32 [], replicated, may hold values from 630784 to 5046272
Outputs:
- loss: float32 [], replicated
- token_grad: float32 [14336, 1024], P('space', 'tensor')
- first_grad: float32 [1024, 1024], P('space', 'tensor')
- second_grad: float32 [1024, 1024], P('space', 'tensor')
- head_grad: float32 [352, 1024], P('tensor', 'space')
The draws below stay inside these ranges and needn't reach their ends.
Inputs may be any that keep to these rules, and one draw needn't show every extreme that they name: `land_mask`: every aligned group of 8 entries along the last dimension holds at least one 1 and one 0. `variable_kind`: 0 scores a variable on all cells, 1 on land cells, 2 on ocean cells.
All inputs are finite; a program needn't handle non-finite values.
Results may differ from the reference program's by a relative error of at most 0.0056.
Values may be sent and summed in bfloat16 or wider, within the bound.
A program may use at most 64 MiB of HBM per device.

```python
import math
import jax
import jax.numpy as jnp
from jax import lax

D = 1024
V = 88
PP = 4
LONP = 224
TOKENS = 14336
COLS = 352


def draw_land_mask(key, part):
    level_key = jax.random.fold_in(key, 21)
    band_key = jax.random.fold_in(key, 22)
    sector_key = jax.random.fold_in(key, 23)
    cell_key = jax.random.fold_in(key, 24)
    first = jax.random.fold_in(key, 25)
    second = jax.random.fold_in(key, 26)
    low_level = jax.random.randint(jax.random.fold_in(level_key, 1), (), 4, 21)
    high_level = jax.random.randint(jax.random.fold_in(level_key, 2), (), 55, 76)
    picker = jax.random.randint(jax.random.fold_in(level_key, 3), (), 0, 2)
    level = jnp.where(picker == 0, low_level, high_level).astype(jnp.int32)
    band_count = TOKENS // LONP
    band_shift = jax.random.randint(band_key, (band_count,), -25, 26).astype(jnp.int32)
    sector_shift = jax.random.randint(sector_key, (8,), -15, 16).astype(jnp.int32)
    position = jnp.arange(TOKENS, dtype=jnp.int32)
    band_index = position // LONP
    sector_index = position % LONP // (LONP // 8)
    chance = jnp.clip(level + band_shift[band_index] + sector_shift[sector_index], 2, 95).astype(jnp.int32)
    rolled = jax.random.randint(cell_key, (PP, TOKENS), 0, 100).astype(jnp.int32)
    base = (rolled < chance[None, :]).astype(jnp.int32)
    blocks = TOKENS // 8
    base = base.reshape(PP, blocks, 8)
    where_one = jax.random.randint(first, (PP, blocks, 1), 0, 8).astype(jnp.int32)
    where_zero = (where_one + jax.random.randint(second, (PP, blocks, 1), 1, 8).astype(jnp.int32)) % 8
    places = jnp.arange(8, dtype=jnp.int32)[None, None, :]
    base = jnp.where(places == where_one, 1, base)
    base = jnp.where(places == where_zero, 0, base)
    return base.reshape(PP, TOKENS).astype(jnp.int32)


def with_ends(array, key, low, high):
    shape = array.shape
    place = [jax.random.randint(jax.random.fold_in(key, axis), (), 0, shape[axis]) for axis in range(len(shape))]
    array = array.at[tuple(place)].set(low)
    longest = shape.index(max(shape))
    place[longest] = (place[longest] + 1) % shape[longest]
    return array.at[tuple(place)].set(high)


def raised(entries, own_key, source, target, parts, factor):
    def block_of(dim):
        return (jnp.arange(entries.shape[dim]) // (entries.shape[dim] // parts)).reshape((-1,) + (1,) * (entries.ndim - 1 - dim))

    one_side = jax.random.permutation(own_key, parts)[block_of(target)]
    second = (block_of(target) + parts // 2) % parts
    return jnp.where((block_of(source) == one_side) | (block_of(source) == second), factor * entries, entries)


def block_levels(key, extent, cuts, smallest, high):
    def one(dim, blocks):
        steps = jax.random.uniform(jax.random.fold_in(jax.random.fold_in(key, 6), dim), (blocks,), jnp.float32, smallest / len(cuts), high / len(cuts))
        return jnp.repeat(jnp.exp(steps), extent[dim] // blocks).reshape((-1,) + (1,) * (len(extent) - dim - 1))

    gain = one(*cuts[0])
    for cut in cuts[1:]:
        gain = gain * one(*cut)
    return gain


def gaussian(stream_key, extent, spread, reach, cuts=(), kind=jnp.bfloat16):
    level = block_levels(stream_key, extent, cuts, -0.22, 0.18) if cuts else 1.0
    drawn = jax.random.normal(stream_key, extent, jnp.float32) * spread * level
    return jnp.minimum(jnp.maximum(drawn, -reach), reach).astype(kind)


def bell_draw_with(key, shape, scale, limit, split, heavy, held_as=jnp.bfloat16):
    values = scale * jax.random.normal(key, shape, jnp.float32)
    if split:
        values = values * block_levels(key, shape, split, -0.22, 0.18)
    return jnp.clip(raised(values, jax.random.fold_in(key, 3), *heavy), -limit, limit).astype(held_as)


def setup_inputs(seed: int = 0) -> dict:
    keys = jax.random.split(jax.random.key(seed), 9)
    return {
        "tokens": bell_draw_with(keys[0], (TOKENS, D), 1.0, 6.0, ((0, 16), (1, 2)), (0, 1, 16, 2.0)),
        "first_weight": gaussian(keys[1], (D, D), D ** -0.5, 0.1875, ((1, 2),)),
        "second_weight": gaussian(keys[2], (D, D), D ** -0.5, 0.1875, ((1, 2),)),
        "head_weight": gaussian(keys[3], (COLS, D), D ** -0.5, 0.1875, ((0, 2),)),
        "targets": gaussian(keys[4], (COLS, TOKENS), 1.0, 6.0, ((0, 2), (1, 16)), jnp.float32),
        "land_mask": draw_land_mask(jax.random.fold_in(keys[8], 71), 0),
        "variable_kind": with_ends(jax.random.randint(keys[6], (V,), 0, 3), jax.random.fold_in(keys[6], 1), 0, 2).astype(jnp.int32),
        "loss_scale": jnp.clip(jnp.exp(jax.random.uniform(keys[7], (), jnp.float32, math.log(630784.0), math.log(5046272))), 630784.0, 5046272),
    }


def slope(z):
    cdf = 0.5 * (1.0 + lax.erf(z / math.sqrt(2.0)))
    return cdf + z * jnp.exp(-0.5 * z * z) / math.sqrt(2.0 * math.pi)

def reference(tokens, first_weight, second_weight, head_weight, targets, land_mask, variable_kind, loss_scale):
    pre_one = jnp.dot(tokens, first_weight, preferred_element_type=jnp.float32)
    hidden_one = jax.nn.gelu(pre_one, approximate=False).astype(jnp.bfloat16)
    pre_two = jnp.dot(hidden_one, second_weight, preferred_element_type=jnp.float32)
    hidden_two = jax.nn.gelu(pre_two, approximate=False).astype(jnp.bfloat16)
    predicted = jnp.dot(head_weight, hidden_two.T, preferred_element_type=jnp.float32)
    position = jnp.arange(TOKENS, dtype=jnp.int32)
    cell = jnp.arange(PP, dtype=jnp.int32)
    lat_row = 2 * (position // LONP)[None, :] + (cell // 2)[:, None]
    nlat = 2 * TOKENS // LONP
    cell_weight = jnp.cos(math.pi / 2.0 * (lat_row.astype(jnp.float32) + 0.5) / nlat)
    land = land_mask.astype(jnp.float32)
    kind = variable_kind[:, None, None]
    valid = jnp.where(kind == 0, 1.0, jnp.where(kind == 1, land[None], 1.0 - land[None])).astype(jnp.float32)
    masked = cell_weight[None] * valid
    error = predicted.reshape(V, PP, TOKENS) - targets.reshape(V, PP, TOKENS)
    weight_sum = lax.optimization_barrier(jnp.sum(masked, axis=(1, 2)))
    error_sum = lax.optimization_barrier(jnp.sum(masked * error * error, axis=(1, 2)))
    root = jnp.sqrt(error_sum / weight_sum + 1e-06)
    loss = jnp.mean(root)
    coef = loss_scale / (V * root * weight_sum)
    grad_pred = (coef[:, None, None] * masked * error).reshape(COLS, TOKENS).astype(jnp.bfloat16)
    head_grad = jnp.dot(grad_pred, hidden_two, preferred_element_type=jnp.float32)
    back_two = jnp.dot(grad_pred.T, head_weight, preferred_element_type=jnp.float32)
    grad_two = (back_two * slope(pre_two)).astype(jnp.bfloat16)
    second_grad = jnp.dot(hidden_one.T, grad_two, preferred_element_type=jnp.float32)
    back_one = jnp.dot(grad_two, second_weight.T, preferred_element_type=jnp.float32)
    grad_one = (back_one * slope(pre_one)).astype(jnp.bfloat16)
    first_grad = jnp.dot(tokens.T, grad_one, preferred_element_type=jnp.float32)
    token_grad = jnp.dot(grad_one, first_weight.T, preferred_element_type=jnp.float32)
    return (loss, token_grad, first_grad, second_grad, head_grad)
```

```python
import math

import jax
import jax.numpy as jnp
from jax import lax
from jax.experimental import pallas as pl
from jax.experimental.pallas import tpu as pltpu
from jax.sharding import PartitionSpec as P

PP = 4
PROW_DEV = 4
LONP = 224
MESH = pl.DeviceIdType.MESH
VMEM = pl.BlockSpec(memory_space=pltpu.VMEM)
ANY = pl.BlockSpec(memory_space=pl.ANY)


def bent(z):
    return (0.5 * z * (1.0 + lax.erf(z / math.sqrt(2.0)))).astype(jnp.bfloat16)


def slope(z):
    cdf = 0.5 * (1.0 + lax.erf(z / math.sqrt(2.0)))
    return cdf + z * jnp.exp(-0.5 * z * z) / math.sqrt(2.0 * math.pi)


def flipped(s, bit):
    step = 1 << bit
    return s + step - 2 * step * ((s // step) % 2)


def greet(partners):
    barrier = pltpu.get_barrier_semaphore()
    for partner in partners:
        pl.semaphore_signal(barrier, inc=1, device_id=partner, device_id_type=MESH)
    pl.semaphore_wait(barrier, len(partners))


def params(number, mib):
    return pltpu.CompilerParams(
        collective_id=number, has_side_effects=True, vmem_limit_bytes=mib * 2**20
    )


TILE = 128
RELAYS = (
    (0, 0), (1, 0), (2, 0), (0, 8), (0, 4), (1, 8), (0, 2), (2, 8), (1, 4), (0, 12), (2, 4),
    (0, 10), (1, 2), (1, 12), (2, 2), (2, 12), (0, 6), (0, 14),
)
CORE_SIDE = (1, 9, 5, 13, 3, 11, 7, 15)
PLAN = ("y", "y", "z", "y", "z")


def fused_kernel(
    scale, label, land, tok, one, two, head, tar,
    o_loss, o_tok, o_one, o_two, o_head,
    w_one, w_two, w_head, toks, tok_out, tar_v, tar_s, tar_all, lnd, masked,
    pre_one, pre_two, h_one, h_two, t_tok, t_one, t_two, tgt, scored, sc_low, sc_par, gp_low,
    g_two, g_one, p_two, p_one, tg_out, hb,
    msg, near, far, mid,
    fars, arrs0, nears0, fars1, arrs1, nears1, fars2, arrs2, nears2, finals, arrs3, arrs4, arrs5,
    local, wsend, wrecv, xsend, xrecv, dsend, drecv, tsend, trecv, rsend, rrecv,
):
    low, wide = jnp.bfloat16, jnp.float32
    s, x = lax.axis_index("space"), lax.axis_index("tensor")
    other = 1 - x
    zf, zn, yy, core = (s // 8) % 2, (s // 4) % 2, (s // 2) % 2, s % 2
    oc = 1 - core
    count = tok.shape[0]
    half = count // 2
    dim, width = one.shape
    rows = head.shape[0]
    pad = toks.shape[0]
    vw = 2 * TILE
    hr = TILE // 2
    across, partner = (s, other), (flipped(s, 0), x)
    diagonal = (flipped(flipped(s, 3), 0), x)
    started = []

    def at(index, size, base=0):
        return pl.ds(pl.multiple_of(index * size + base, math.gcd(size, base) if base else size), size)

    def remote(src, dst, sends, recvs, slot, target):
        copy = pltpu.make_async_remote_copy(
            src_ref=src,
            dst_ref=dst,
            send_sem=sends.at[slot],
            recv_sem=recvs.at[slot],
            device_id=target,
            device_id_type=MESH,
        )
        copy.start()
        started.append(copy)
        return copy

    moves = [
        (one, w_one.at[:, at(x, width)]),
        (two, w_two.at[:, at(x, width)]),
        (head, w_head.at[pl.ds(pl.multiple_of(x * vw, vw), rows), :]),
        (tok.at[at(other, half), :], tok_out),
        (tar, tar_v),
        (tok.at[at(x, half), :], toks.at[pl.ds(0, half), at(x, width)]),
    ]
    loads = [pltpu.make_async_copy(a, b, local.at[n]) for n, (a, b) in enumerate(moves)]
    for copy in loads:
        copy.start()

    shard = 96
    w_head[pl.ds(pl.multiple_of(x * vw + rows, 16), vw - rows), :] = jnp.zeros((vw - rows, dim), low)
    w_head[pl.ds(pl.multiple_of(other * vw + 2 * shard, 16), vw - 2 * shard), :] = jnp.zeros(
        (vw - 2 * shard, dim), low
    )
    for ref in (toks, h_one, h_two, g_two, g_one, sc_low):
        ref[half:, :] = jnp.zeros((pad - half, ref.shape[1]), low)
    tar_all[:, rows:, :] = jnp.zeros((2, vw - rows, pad), low)

    low_bits, high = s % 4, s // 4
    mine = x * 4 + low_bits

    def near_peer(d):
        j = (mine + d) % 8
        return (high * 4 + j % 4, j // 4)

    def far_peer(d):
        return (((high + d) % 4) * 4 + low_bits, x)

    greet([near_peer(d) for d in range(1, 8)] + [far_peer(d) for d in range(1, 4)] + [diagonal])

    part = dim // 16

    def place(k, m, side):
        q = s
        for b in range(4):
            if (m >> b) & 1:
                q = flipped(q, b)
        if k < 2:
            return (w_one, w_two)[k].at[at(q, part), at(side, width)]
        first = pl.multiple_of(side * vw + (q % 2) * shard, 16)
        return w_head.at[pl.ds(first, shard), at(q // 2, TILE)]

    pieces = {}
    for k in range(3):
        loads[k].wait()
        pieces[k, 0] = remote(place(k, 0, x), place(k, 0, x), wsend, wrecv, 16 * k, across)
    loads[3].wait()
    parts = 2
    step = half // parts
    tok_copies = [
        remote(
            tok_out.at[pl.ds(n * step, step), :],
            toks.at[pl.ds(n * step, step), at(x, width)],
            xsend, xrecv, n, across,
        )
        for n in range(parts)
    ]
    loads[4].wait()
    tail = count - pad
    spare = lax.broadcasted_iota(jnp.int32, (rows, pad), 1) >= half
    tags = jnp.concatenate([label[...]] * (pad // TILE), axis=1)
    lo = tar_v[:, :pad]
    hi = pltpu.roll(tar_v[:, tail:], pad - half + tail, 1)
    tar_s[...] = jnp.where(spare, tags, jnp.where(x == 0, hi, lo)).astype(low)
    tar_copy = remote(tar_s, tar_all.at[x, pl.ds(0, rows), :], xsend, xrecv, parts, across)
    tar_all[x, 0:rows, :] = jnp.where(spare, tags, jnp.where(x == 0, lo, hi)).astype(low)
    loads[5].wait()

    def relay(k, m):
        pieces[k, m].wait_recv()
        for b in (3, 2, 1, 0):
            if m & ((2 << b) - 1) == 0:
                piece = place(k, m, other)
                new = m ^ (1 << b)
                pieces[k, new] = remote(piece, piece, wsend, wrecv, 16 * k + new, (flipped(s, b), x))

    for k, m in RELAYS:
        relay(k, m)
    for m in CORE_SIDE:
        relay(0, m)

    def one_rows(first, size):
        def body(n, _):
            z = jnp.dot(toks[first : first + size, :], w_one[:, at(n, vw)], preferred_element_type=wide)
            pre_one[first : first + size, at(n, vw)] = z
            h_one[first : first + size, at(n, vw)] = bent(z)
            return 0

        lax.fori_loop(0, dim // vw, body, 0)

    for n in range(parts):
        tok_copies[n].wait_recv()
        one_rows(n * step, step)
    for k, m in ((1, 10), (2, 10), (1, 6), (1, 14), (2, 6), (2, 14)):
        relay(k, m)
    for m in CORE_SIDE:
        relay(1, m)

    def two_body(n, _):
        z = jnp.dot(h_one[0:half, :], w_two[:, at(n, vw)], preferred_element_type=wide)
        pre_two[:, at(n, vw)] = z
        h_two[0:half, at(n, vw)] = bent(z)
        return 0

    lax.fori_loop(0, dim // vw, two_body, 0)
    for m in CORE_SIDE:
        relay(2, m)
    tar_copy.wait_recv()

    for side in range(2):
        tgt[:, side * vw : (side + 1) * vw] = tar_all[side].astype(wide).T
    lane = lax.broadcasted_iota(jnp.int32, (1, 2 * vw), 1)
    used = lane % vw < rows
    kind = tgt[half : half + 1, :]
    cell = lane % PP
    lnd[...] = jnp.zeros_like(lnd)
    lnd[0:PP, :] = land[...].astype(wide)
    ground = jnp.where(x == 0, lnd[:, :pad], pltpu.roll(lnd[:, tail:], pad - half + tail, 1))
    pick_shape = (TILE, 2 * vw)
    pick = lax.broadcasted_iota(jnp.int32, pick_shape, 1) % PP == lax.broadcasted_iota(jnp.int32, pick_shape, 0)
    spread = jnp.dot(
        ground.T.astype(low), jnp.where(pick, 1.0, 0.0).astype(low), preferred_element_type=wide
    )
    bands = half // LONP
    nlat = 2 * (count // LONP) * lax.axis_size("space")
    for j in range(bands):
        lat_row = 2 * (s * (count // LONP) + x * bands + j) + cell // 2
        weight = jnp.cos(math.pi / 2.0 * (lat_row.astype(wide) + 0.5) / nlat)
        weight = jnp.where(used, weight, 0.0)
        flat = jnp.where(kind == 1.0, 0.0, weight)
        slant = jnp.where(kind == 1.0, weight, jnp.where(kind == 2.0, -weight, 0.0))
        band = slice(j * LONP, (j + 1) * LONP)
        masked[band, :] = flat + slant * spread[band, :]

    for side in range(2):
        cols = slice(side * vw, (side + 1) * vw)
        error = lax.dot_general(
            h_two[0:half, :], w_head[cols, :], (((1,), (1,)), ((), ())), preferred_element_type=wide
        )
        error = error - tgt[0:half, cols]
        m = masked[:, cols]
        sc = m * error
        scored[:, cols] = sc
        sc_low[0:half, cols] = sc.astype(low)
        esum = jnp.sum(sc * error, axis=0, keepdims=True)
        wsum = jnp.sum(m, axis=0, keepdims=True)
        for n in range(2):
            r = side * 2 + n
            msg[r : r + 1, :] = esum[:, n * TILE : (n + 1) * TILE]
            msg[4 + r : 5 + r, :] = wsum[:, n * TILE : (n + 1) * TILE]

    def share(src, slots, me, peers, base):
        copies = [remote(src, slots.at[me], tsend, trecv, base + n, peer) for n, peer in enumerate(peers)]
        slots[me] = src[...]
        return copies

    first_share = share(msg, near, mine, [near_peer(d) for d in range(1, 8)], 0)

    def scored_cols(side, c):
        return pl.ds(pl.multiple_of(side * vw + c * TILE, TILE), TILE)

    score_copies = [
        remote(sc_low.at[:, scored_cols(n, oc)], sc_par.at[:, pl.ds(n * TILE, TILE)], dsend, drecv, n, partner)
        for n in range(2)
    ]

    def flip_to(src, dst, slot):
        def body(n, _):
            dst[0, at(n, TILE), :] = src[:, at(n, TILE)].T
            return 0

        lax.fori_loop(0, dim // TILE, body, 0)
        return remote(dst.at[0], dst.at[1], dsend, drecv, slot, partner)

    flips = [flip_to(h_two, t_two, 2)]
    for copy in first_share:
        copy.wait_recv()
    mid[...] = jnp.sum(near[...], axis=0)
    second_share = share(mid, far, high, [far_peer(d) for d in range(1, 4)], 7)
    flips += [flip_to(h_one, t_one, 3), flip_to(toks, t_tok, 4)]

    def make_slope(ref):
        def body(n, _):
            ref[:, at(n, TILE)] = slope(ref[:, at(n, TILE)])
            return 0

        lax.fori_loop(0, dim // TILE, body, 0)

    ways = {"z": (zn, 2), "y": (yy, 1)}

    def produce(g, trans, own_cols, par_cols):
        value, bit = ways[PLAN[g]]

        def product(v):
            def side_rows(k):
                blocks = []
                for i in range(2):
                    for j in range(2):
                        index = i * 4 + (j * 2 + v if PLAN[g] == "y" else v * 2 + j)
                        blocks.append(trans[k, at(index, TILE), :])
                return jnp.concatenate(blocks, axis=0)

            out = jnp.dot(side_rows(0), own_cols, preferred_element_type=wide)
            out += jnp.dot(side_rows(1), par_cols, preferred_element_type=wide)
            return out.reshape(2, 2, TILE, vw)

        fars[g] = product(1 - value).astype(low)
        copy = remote(fars.at[g], arrs0.at[g], rsend, rrecv, 6 * g, (flipped(s, bit), x))
        nears0[g] = product(value)
        return copy

    def advance_one(g, copy):
        copy.wait_recv()
        value, bit = ways["z" if PLAN[g] == "y" else "y"]
        fars1[g] = (nears0[g, :, 1 - value] + arrs0[g, :, 1 - value].astype(wide)).astype(low)
        copy = remote(fars1.at[g], arrs1.at[g], rsend, rrecv, 6 * g + 1, (flipped(s, bit), x))
        nears1[g] = nears0[g, :, value] + arrs0[g, :, value].astype(wide)
        return copy

    def advance_two(g, copy):
        copy.wait_recv()
        away, here = at(other, TILE), at(x, TILE)
        fars2[g] = (nears1[g, :, :, away] + arrs1[g, :, :, away].astype(wide)).astype(low)
        copy = remote(fars2.at[g], arrs2.at[g], rsend, rrecv, 6 * g + 2, across)
        nears2[g] = nears1[g, :, :, here] + arrs1[g, :, :, here].astype(wide)
        return copy

    def advance_three(g, copy):
        copy.wait_recv()
        finals[g] = (nears2[g, 1 - zf] + arrs2[g, 1 - zf].astype(wide)).astype(low)
        up = (flipped(s, 3), x)
        copies = [
            remote(finals.at[g, at(core, hr), :], arrs4.at[g], rsend, rrecv, 6 * g + 3, up),
            remote(finals.at[g, at(oc, hr), :], arrs5.at[g], rsend, rrecv, 6 * g + 4, diagonal),
        ]
        nears2[g, zf] = nears2[g, zf] + arrs2[g, zf].astype(wide)
        copies.append(
            remote(nears2.at[g, zf, at(oc, hr), :], arrs3.at[g], rsend, rrecv, 6 * g + 5, partner)
        )
        return copies

    def finish(g, copies, out, base):
        for copy in copies:
            copy.wait_recv()
        kept = nears2[g, zf, at(core, hr), :] + arrs4[g].astype(wide)
        came = arrs3[g] + arrs5[g].astype(wide)
        span = out.shape[1] // 2
        out[pl.ds(0, hr), pl.ds(pl.multiple_of(core * span + base, TILE), TILE)] = kept
        out[pl.ds(0, hr), pl.ds(pl.multiple_of(oc * span + base, TILE), TILE)] = came

    for copy in score_copies:
        copy.wait_recv()
    flips[0].wait_recv()
    state = {}
    own = jnp.concatenate([sc_low[:, scored_cols(n, core)] for n in range(2)], axis=1)
    state[0] = produce(0, t_two, own, sc_par[...])
    make_slope(pre_two)

    for copy in second_share:
        copy.wait_recv()
    sums = jnp.sum(far[...], axis=0)
    tl = lax.broadcasted_iota(jnp.int32, (8, TILE), 1)
    sums = sums + jnp.where(tl % 2 == 0, pltpu.roll(sums, TILE - 1, 1), pltpu.roll(sums, 1, 1))
    sums = sums + jnp.where(tl % 4 < 2, pltpu.roll(sums, TILE - 2, 1), pltpu.roll(sums, 2, 1))
    kinds = 2 * rows // PP
    line = lax.broadcasted_iota(jnp.int32, (4, TILE), 0)
    tl = lax.broadcasted_iota(jnp.int32, (4, TILE), 1)
    ok = (line % 2) * TILE + tl < rows
    weight_sum = jnp.where(ok, sums[4:8, :], 1.0)
    root = jnp.sqrt(jnp.where(ok, sums[0:4, :], 0.0) / weight_sum + 1e-06)
    roots = jnp.where(ok & (tl % PP == 0), root, 0.0)
    loss = jnp.sum(jnp.sum(roots, axis=0, keepdims=True), axis=1, keepdims=True) / kinds
    o_loss[...] = jnp.broadcast_to(loss, o_loss.shape)
    coef = jnp.where(ok, scale[0] / (kinds * root * weight_sum), 0.0)
    coef = jnp.concatenate([coef[n : n + 1, :] for n in range(4)], axis=1)
    gp_low[...] = (coef * scored[...]).astype(low)

    def grad_tiles(made, send_to, base, make):
        copies = []
        for c in (oc, core):
            for side in range(2):
                tile = pl.ds(pl.multiple_of(side * width + c * vw, vw), vw)
                made[0:half, tile] = make(tile)
                if c is oc:
                    copies.append(
                        remote(
                            made.at[:, tile], send_to.at[:, pl.ds(side * vw, vw)],
                            dsend, drecv, base + side, partner,
                        )
                    )
        return copies

    def make_two(tile):
        b = jnp.dot(gp_low[...], w_head[:, tile], preferred_element_type=wide)
        return (b * pre_two[:, tile]).astype(low)

    two_copies = grad_tiles(g_two, p_two, 5, make_two)
    make_slope(pre_one)

    def make_one(tile):
        b = lax.dot_general(
            g_two[0:half, :], w_two[tile, :], (((1,), (1,)), ((), ())), preferred_element_type=wide
        )
        return (b * pre_one[:, tile]).astype(low)

    one_copies = grad_tiles(g_one, p_one, 7, make_one)

    def both(made, came, a):
        own_cols = [
            made[:, pl.ds(pl.multiple_of(n * width + core * vw + a * TILE, TILE), TILE)] for n in range(2)
        ]
        par_cols = [came[:, n * vw + a * TILE : n * vw + (a + 1) * TILE] for n in range(2)]
        return jnp.concatenate(own_cols, axis=1), jnp.concatenate(par_cols, axis=1)

    for copy in two_copies + [flips[1]]:
        copy.wait_recv()
    for a in range(2):
        state[1 + a] = produce(1 + a, t_one, *both(g_two, p_two, a))
    state[0] = advance_one(0, state[0])
    for copy in one_copies + [flips[2]]:
        copy.wait_recv()
    for a in range(2):
        state[3 + a] = produce(3 + a, t_tok, *both(g_one, p_one, a))
    state[0] = advance_two(0, state[0])

    def token_side(side, write):
        for n in range(width // vw):
            b = lax.dot_general(
                g_one[0:half, :],
                w_one[pl.ds(pl.multiple_of(side * width + n * vw, vw), vw), :],
                (((1,), (1,)), ((), ())),
                preferred_element_type=wide,
            )
            write(n, b.astype(low))

    def write_far(n, b):
        tg_out[:, n * vw : (n + 1) * vw] = b

    def write_near(n, b):
        o_tok[at(x, half), n * vw : (n + 1) * vw] = b

    token_side(other, write_far)
    tg_copy = remote(tg_out, o_tok.at[at(x, half), :], xsend, xrecv, parts + 1, across)
    state[1] = advance_one(1, state[1])
    state[2] = advance_one(2, state[2])
    token_side(x, write_near)
    state[0] = advance_three(0, state[0])
    state[3] = advance_one(3, state[3])
    state[1] = advance_two(1, state[1])
    state[2] = advance_two(2, state[2])
    state[4] = advance_one(4, state[4])
    finish(0, state[0], hb, 0)
    coef_here = jnp.where(x == 0, coef[:, :vw], coef[:, vw:])
    o_head[...] = (hb[...] * coef_here).T[0:rows, 0:hr]
    state[1] = advance_three(1, state[1])
    state[2] = advance_three(2, state[2])
    state[3] = advance_two(3, state[3])
    state[4] = advance_two(4, state[4])
    finish(1, state[1], o_two, 0)
    finish(2, state[2], o_two, TILE)
    state[3] = advance_three(3, state[3])
    state[4] = advance_three(4, state[4])
    finish(3, state[3], o_one, 0)
    finish(4, state[4], o_one, TILE)
    tg_copy.wait_recv()
    for copy in started:
        copy.wait_send()


def fused(scale, label, land, tokens, first, second, head, targets):
    count, width = tokens.shape
    dim = first.shape[0]
    rows = head.shape[0]
    half = count // 2
    pad = -(-(half + 1) // TILE) * TILE
    vw = 2 * TILE
    hr = TILE // 2
    low, wide = jnp.bfloat16, jnp.float32
    shape = jax.ShapeDtypeStruct
    slices = len(PLAN)
    vm = pltpu.VMEM
    scratch = [
        vm((dim, dim), low), vm((dim, dim), low), vm((2 * vw, dim), low), vm((pad, dim), low),
        vm((half, width), low), vm((rows, count), wide), vm((rows, pad), low), vm((2, vw, pad), low),
        vm((TILE, count), wide), vm((half, 2 * vw), wide),
        vm((half, dim), wide), vm((half, dim), wide), vm((pad, dim), low), vm((pad, dim), low),
        vm((2, dim, pad), low), vm((2, dim, pad), low), vm((2, dim, pad), low),
        vm((pad, 2 * vw), wide), vm((half, 2 * vw), wide), vm((pad, 2 * vw), low), vm((pad, vw), low),
        vm((half, 2 * vw), low),
        vm((pad, dim), low), vm((pad, dim), low), vm((pad, width), low), vm((pad, width), low),
        vm((half, width), low), vm((TILE, vw), wide),
        vm((8, TILE), wide), vm((8, 8, TILE), wide), vm((4, 8, TILE), wide), vm((8, TILE), wide),
        vm((slices, 2, 2, TILE, vw), low), vm((slices, 2, 2, TILE, vw), low), vm((slices, 2, 2, TILE, vw), wide),
        vm((slices, 2, TILE, vw), low), vm((slices, 2, TILE, vw), low), vm((slices, 2, TILE, vw), wide),
        vm((slices, 2, TILE, TILE), low), vm((slices, 2, TILE, TILE), low), vm((slices, 2, TILE, TILE), wide),
        vm((slices, TILE, TILE), low), vm((slices, hr, TILE), wide),
        vm((slices, hr, TILE), low), vm((slices, hr, TILE), low),
    ]
    sizes = (6, 48, 48, 4, 4, 9, 9, 10, 10, 6 * slices, 6 * slices)
    scratch += [pltpu.SemaphoreType.DMA((n,)) for n in sizes]
    return pl.pallas_call(
        fused_kernel,
        out_shape=(
            shape((8, TILE), wide),
            shape((count, width), low),
            shape((dim // 16, width), wide),
            shape((dim // 16, width), wide),
            shape((rows, hr), wide),
        ),
        in_specs=[pl.BlockSpec(memory_space=pltpu.SMEM), VMEM, VMEM] + [ANY] * 5,
        out_specs=[VMEM] * 5,
        scratch_shapes=scratch,
        compiler_params=params(0, 56),
        name="fused",
    )(scale, label, land, tokens, first, second, head, targets)


def per_device(
    tokens, first_weight, second_weight, head_weight, targets, land_mask, variable_kind, loss_scale
):
    rows = head_weight.shape[0]
    label = jnp.repeat(variable_kind, PP).astype(jnp.float32)[:, None]
    label = jnp.broadcast_to(label, (rows, TILE))
    loss, token_grad, first_grad, second_grad, head_grad = fused(
        loss_scale.reshape(1), label, land_mask, tokens, first_weight, second_weight, head_weight, targets
    )
    return (loss[0, 0], token_grad.astype(jnp.float32), first_grad, second_grad, head_grad)


def column_folder(weights, piece):
    return lax.dot_general(
        piece, weights, (((1,), (1,)), ((), ())), preferred_element_type=jnp.float32
    )


def row_folder(weights, piece):
    return lax.dot_general(
        piece, weights, (((0,), (0,)), ((), ())), preferred_element_type=jnp.float32
    )


def per_device_wide(
    tokens, first_weight, second_weight, head_weight, targets, land_mask, variable_kind, loss_scale
):
    count = tokens.shape[0]
    width = first_weight.shape[1]
    kinds = head_weight.shape[0] // PP
    rows_first, rows_second = (
        lax.all_to_all(first_weight, "tensor", split_axis=0, concat_axis=1, tiled=True),
        lax.all_to_all(second_weight, "tensor", split_axis=0, concat_axis=1, tiled=True),
    )
    head_cols = lax.all_to_all(head_weight, "tensor", split_axis=1, concat_axis=0, tiled=True)
    position = lax.axis_index("space") * count + jnp.arange(count, dtype=jnp.int32)
    cell = jnp.arange(PP, dtype=jnp.int32)
    lat_row = 2 * (position // LONP)[None, :] + (cell // 2)[:, None]
    nlat = 2 * PROW_DEV * lax.axis_size("space")
    cell_weight = jnp.cos(math.pi / 2.0 * (lat_row.astype(jnp.float32) + 0.5) / nlat)
    land = land_mask.astype(jnp.float32)
    kind = variable_kind[:, None, None]
    valid = jnp.where(kind == 0, 1.0, jnp.where(kind == 1, land[None], 1.0 - land[None]))
    masked = cell_weight[None] * valid
    local_weight = jnp.sum(masked, axis=(1, 2))
    weight_sum = lax.psum(local_weight, "space")
    full_in = lax.all_gather(tokens, "tensor", axis=1, tiled=True)
    pre_one = jnp.dot(full_in, first_weight, preferred_element_type=jnp.float32)
    hidden_one = jax.nn.gelu(pre_one, approximate=False).astype(jnp.bfloat16)
    full_one = lax.all_gather(hidden_one, "tensor", axis=1, tiled=True)
    pre_two = jnp.dot(full_one, second_weight, preferred_element_type=jnp.float32)
    hidden_two = jax.nn.gelu(pre_two, approximate=False).astype(jnp.bfloat16)
    full_two = lax.all_gather(hidden_two, "tensor", axis=1, tiled=True)
    predicted = lax.dot_general(
        head_weight, full_two, (((1,), (1,)), ((), ())), preferred_element_type=jnp.float32
    )
    error = predicted.reshape(kinds, PP, count) - targets.reshape(kinds, PP, count)
    local_error = jnp.sum(masked * error * error, axis=(1, 2))
    error_sum = lax.psum(local_error, "space")
    root = jnp.sqrt(error_sum / weight_sum + 1e-06)
    loss = lax.psum(jnp.sum(root), "tensor") / (kinds * lax.axis_size("tensor"))
    coef = loss_scale / (kinds * lax.axis_size("tensor") * root * weight_sum)
    grad_pred = (
        (coef[:, None, None] * masked * error).reshape(kinds * PP, count).astype(jnp.bfloat16)
    )
    back_two = row_folder(head_cols, lax.all_gather(grad_pred, "tensor", axis=0, tiled=True))
    head_term = jnp.dot(grad_pred, full_two, preferred_element_type=jnp.float32)
    head_grad = lax.psum_scatter(head_term, "space", scatter_dimension=1, tiled=True)
    grad_two = (back_two * slope(pre_two)).astype(jnp.bfloat16)
    back_one = column_folder(rows_second, lax.all_gather(grad_two, "tensor", axis=1, tiled=True))
    grad_one = (back_one * slope(pre_one)).astype(jnp.bfloat16)
    joined = lax.psum_scatter(
        jnp.concatenate(
            [
                lax.dot_general(
                    full_one, grad_two, (((0,), (0,)), ((), ())), preferred_element_type=jnp.float32
                ),
                lax.dot_general(
                    full_in, grad_one, (((0,), (0,)), ((), ())), preferred_element_type=jnp.float32
                ),
            ],
            axis=1,
        ),
        "space",
        scatter_dimension=0,
        tiled=True,
    )
    second_grad = joined[:, :width]
    first_grad = joined[:, width:]
    token_grad = column_folder(rows_first, lax.all_gather(grad_one, "tensor", axis=1, tiled=True))
    return (loss, token_grad, first_grad, second_grad, head_grad)


def solution(mesh):
    size = mesh.shape["space"]
    paired = mesh.shape["tensor"] == 2 and size == 16
    return jax.shard_map(
        per_device if paired else per_device_wide,
        mesh=mesh,
        in_specs=(
            P("space", "tensor"),
            P(None, "tensor"),
            P(None, "tensor"),
            P("tensor", None),
            P("tensor", "space"),
            P(None, "space"),
            P("tensor"),
            P(),
        ),
        out_specs=(
            P(),
            P("space", "tensor"),
            P("space", "tensor"),
            P("space", "tensor"),
            P("tensor", "space"),
        ),
        check_vma=False,
    )
```

```python
import math

import jax
import jax.numpy as jnp
from jax import lax
from jax.experimental import pallas as pl
from jax.experimental.pallas import tpu as pltpu
from jax.sharding import PartitionSpec as P

PP = 4
PROW_DEV = 4
LONP = 224
MESH = pl.DeviceIdType.MESH
VMEM = pl.BlockSpec(memory_space=pltpu.VMEM)
ANY = pl.BlockSpec(memory_space=pl.ANY)


def bent(z):
    return (0.5 * z * (1.0 + lax.erf(z / math.sqrt(2.0)))).astype(jnp.bfloat16)


def slope(z):
    cdf = 0.5 * (1.0 + lax.erf(z / math.sqrt(2.0)))
    return cdf + z * jnp.exp(-0.5 * z * z) / math.sqrt(2.0 * math.pi)


def flipped(s, bit):
    step = 1 << bit
    return s + step - 2 * step * ((s // step) % 2)


def greet(partners):
    barrier = pltpu.get_barrier_semaphore()
    for partner in partners:
        pl.semaphore_signal(barrier, inc=1, device_id=partner, device_id_type=MESH)
    pl.semaphore_wait(barrier, len(partners))


def params(number, mib):
    return pltpu.CompilerParams(
        collective_id=number, has_side_effects=True, vmem_limit_bytes=mib * 2**20
    )


TILE = 128
TREES = ((2, 1, 0), (3, 2, 1, 0), (1, 3, 2, 0))
PLAN = (("y", "x", "z"), ("y", "z", "x"), ("z", "y", "x"), ("y", "x", "z"), ("z", "y", "x"))
BITS = {"z": 2, "y": 1}


def stage_shapes(order):
    found = []
    lead, lanes = 2, 2 * TILE
    for way in order[1:]:
        found.append((2,) * lead + (TILE, lanes))
        if way == "x":
            lanes = TILE
        else:
            lead -= 1
    found.append((2,) * lead + (TILE, lanes))
    return found


def fused_kernel(
    scale, kinds_in, land, tok, one, two, head, tar,
    o_loss, o_tok, o_one, o_two, o_head,
    w_one, w_two, w_head, toks, tok_out, tar_v, tar_s, tar_all, lnd, masked,
    pre_one, pre_two, h_one, h_two, t_tok, t_one, t_two, tgt, scored, sc_low, sc_par, gp_low,
    g_two, g_one, p_two, p_one, tg_far, tg_near, r_one, r_two, r_head, hb, r_loss, kb, kp,
    msg, near, far, mid, finals, arrs3, arrs4, arrs5, *refs,
):
    slices = len(PLAN)
    fars, arrs, nears = [[refs[j * 3 * slices + g * 3 : j * 3 * slices + g * 3 + 3] for g in range(slices)] for j in range(3)]
    local, wsend, wrecv, xsend, xrecv, dsend, drecv, tsend, trecv, rsend, rrecv, outs = refs[9 * slices :]
    low, wide = jnp.bfloat16, jnp.float32
    s, x = lax.axis_index("space"), lax.axis_index("tensor")
    other = 1 - x
    zf, zn, yy, core = (s // 8) % 2, (s // 4) % 2, (s // 2) % 2, s % 2
    oc = 1 - core
    count = tok.shape[0]
    half = count // 2
    dim, width = one.shape
    rows = head.shape[0]
    pad = toks.shape[0]
    vw = 2 * TILE
    hr = TILE // 2
    across, partner = (s, other), (flipped(s, 0), x)
    diagonal = (flipped(flipped(s, 3), 0), x)
    started, writes = [], []

    def at(index, size):
        return pl.ds(pl.multiple_of(index * size, size), size)

    def remote(src, dst, sends, recvs, slot, target):
        copy = pltpu.make_async_remote_copy(
            src_ref=src,
            dst_ref=dst,
            send_sem=sends.at[slot],
            recv_sem=recvs.at[slot],
            device_id=target,
            device_id_type=MESH,
        )
        copy.start()
        started.append(copy)
        return copy

    def write_out(src, dst):
        copy = pltpu.make_async_copy(src, dst, outs.at[len(writes)])
        copy.start()
        writes.append(copy)

    moves = [
        (one, w_one.at[:, at(x, width)]),
        (two, w_two.at[:, at(x, width)]),
        (head, w_head.at[pl.ds(pl.multiple_of(x * vw, vw), rows), :]),
        (tok.at[at(other, half), :], tok_out),
        (tar, tar_v),
        (tok.at[at(x, half), :], toks.at[pl.ds(0, half), at(x, width)]),
    ]
    loads = [pltpu.make_async_copy(a, b, local.at[n]) for n, (a, b) in enumerate(moves)]
    for copy in loads:
        copy.start()

    shard = 96
    w_head[pl.ds(pl.multiple_of(x * vw + rows, 16), vw - rows), :] = jnp.zeros((vw - rows, dim), low)
    w_head[pl.ds(pl.multiple_of(other * vw + 2 * shard, 16), vw - 2 * shard), :] = jnp.zeros(
        (vw - 2 * shard, dim), low
    )
    for ref in (toks, h_one, h_two, g_two, g_one, sc_low):
        ref[half:, :] = jnp.zeros((pad - half, ref.shape[1]), low)
    tar_all[:, rows:, :] = jnp.zeros((2, vw - rows, pad), low)
    kb[...] = jnp.zeros_like(kb)
    kb[0:1, 0 : rows // PP] = kinds_in[...].astype(wide)
    lnd[...] = jnp.zeros_like(lnd)
    lnd[0:PP, :] = land[...].astype(wide)

    low_bits, high = s % 4, s // 4
    mine = x * 4 + low_bits

    def near_peer(d):
        j = (mine + d) % 8
        return (high * 4 + j % 4, j // 4)

    def far_peer(d):
        return (((high + d) % 4) * 4 + low_bits, x)

    greet([near_peer(d) for d in range(1, 8)] + [far_peer(d) for d in range(1, 4)] + [diagonal])

    part = dim // 16

    def place(k, m, side):
        q = s
        for b in range(4):
            if (m >> b) & 1:
                q = flipped(q, b)
        if k == 0:
            return w_one.at[at(q % 8, 2 * part), at(side, width)]
        if k == 1:
            return w_two.at[at(q, part), at(side, width)]
        first = pl.multiple_of(side * vw + (q % 2) * shard, 16)
        return w_head.at[pl.ds(first, shard), at(q // 2, TILE)]

    pieces = {}
    for k in range(3):
        loads[k].wait()
        pieces[k, 0] = remote(place(k, 0, x), place(k, 0, x), wsend, wrecv, 16 * k, across)
    kind_copy = remote(kb, kp, xsend, xrecv, 4, across)
    loads[3].wait()
    parts = 2
    step = half // parts
    tok_copies = [
        remote(
            tok_out.at[pl.ds(n * step, step), :],
            toks.at[pl.ds(n * step, step), at(x, width)],
            xsend, xrecv, n, across,
        )
        for n in range(parts)
    ]
    loads[4].wait()
    tail = count - pad
    lo = tar_v[:, :pad]
    hi = pltpu.roll(tar_v[:, tail:], pad - half + tail, 1)
    tar_s[...] = jnp.where(x == 0, hi, lo).astype(low)
    tar_copy = remote(tar_s, tar_all.at[x, pl.ds(0, rows), :], xsend, xrecv, parts, across)
    tar_all[x, 0:rows, :] = jnp.where(x == 0, lo, hi).astype(low)
    loads[5].wait()

    def relay(k, *ms):
        for m in ms:
            pieces[k, m].wait_recv()
            last = -1
            for n, b in enumerate(TREES[k]):
                if (m >> b) & 1:
                    last = n
            for b in TREES[k][last + 1 :]:
                piece = place(k, m, other)
                new = m ^ (1 << b)
                pieces[k, new] = remote(piece, piece, wsend, wrecv, 16 * k + new, (flipped(s, b), x))

    def layer(src, first, size, weight, side, pre, dst):
        span = slice(first, first + size)
        for i in range(width // vw):
            tile = pl.ds(pl.multiple_of(side * width + i * vw, vw), vw)
            z = jnp.dot(src[span, :], weight[:, tile], preferred_element_type=wide)
            pre[span, tile] = z
            dst[span, tile] = bent(z)

    def flip_to(src, dst, slot):
        for n in range(dim // TILE):
            dst[0, n * TILE : (n + 1) * TILE, :] = src[:, n * TILE : (n + 1) * TILE].T
        return remote(dst.at[0], dst.at[1], dsend, drecv, slot, partner)

    def make_slope(ref):
        def body(n, _):
            ref[:, at(n, TILE)] = slope(ref[:, at(n, TILE)])
            return 0

        lax.fori_loop(0, dim // TILE, body, 0)

    relay(0, 0)
    relay(1, 0)
    relay(2, 0)
    kind_copy.wait_recv()
    lane = lax.broadcasted_iota(jnp.int32, (1, 2 * vw), 1)
    used = lane % vw < rows
    cell = lane % PP
    group_shape = (TILE, vw)
    group = lax.broadcasted_iota(jnp.int32, group_shape, 1) // PP == lax.broadcasted_iota(jnp.int32, group_shape, 0)
    group = jnp.where(group, 1.0, 0.0).astype(low)
    k_own = jnp.dot(kb[...].astype(low), group, preferred_element_type=wide)[0:1, :]
    k_oth = jnp.dot(kp[...].astype(low), group, preferred_element_type=wide)[0:1, :]
    kind = jnp.concatenate([jnp.where(x == 0, k_own, k_oth), jnp.where(x == 0, k_oth, k_own)], axis=1)
    ground = jnp.where(x == 0, lnd[:, :pad], pltpu.roll(lnd[:, tail:], pad - half + tail, 1))
    pick_shape = (TILE, 2 * vw)
    pick = lax.broadcasted_iota(jnp.int32, pick_shape, 1) % PP == lax.broadcasted_iota(jnp.int32, pick_shape, 0)
    spread = jnp.dot(
        ground.T.astype(low), jnp.where(pick, 1.0, 0.0).astype(low), preferred_element_type=wide
    )
    bands = half // LONP
    nlat = 2 * (count // LONP) * lax.axis_size("space")
    for j in range(bands):
        lat_row = 2 * (s * (count // LONP) + x * bands + j) + cell // 2
        weight = jnp.cos(math.pi / 2.0 * (lat_row.astype(wide) + 0.5) / nlat)
        weight = jnp.where(used, weight, 0.0)
        flat = jnp.where(kind == 1.0, 0.0, weight)
        slant = jnp.where(kind == 1.0, weight, jnp.where(kind == 2.0, -weight, 0.0))
        band = slice(j * LONP, (j + 1) * LONP)
        masked[band, :] = flat + slant * spread[band, :]
    relay(0, 4, 2)
    relay(1, 2, 4)
    relay(2, 2)
    relay(1, 8)
    tgt[:, at(x, vw)] = tar_all[x].astype(wide).T
    relay(2, 4, 8)
    tok_copies[0].wait_recv()
    layer(toks, 0, step, w_one, x, pre_one, h_one)
    relay(0, 6)
    relay(1, 12)
    relay(2, 6)
    relay(0, 1, 5, 3, 7)
    layer(toks, 0, step, w_one, other, pre_one, h_one)
    relay(1, 6)
    relay(2, 10, 12, 14)
    tok_copies[1].wait_recv()
    layer(toks, step, half - step, w_one, x, pre_one, h_one)
    layer(toks, step, half - step, w_one, other, pre_one, h_one)
    relay(1, 10, 14)
    layer(h_one, 0, half, w_two, x, pre_two, h_two)
    flips = [flip_to(toks, t_tok, 4)]
    relay(1, 1, 9, 5, 13, 3, 11, 7, 15)
    layer(h_one, 0, half, w_two, other, pre_two, h_two)
    relay(2, 1, 9, 5, 13, 3, 11, 7, 15)
    tar_copy.wait_recv()
    tgt[:, at(other, vw)] = tar_all[other].astype(wide).T
    for side in range(2):
        cols = slice(side * vw, (side + 1) * vw)
        error = lax.dot_general(
            h_two[0:half, :], w_head[cols, :], (((1,), (1,)), ((), ())), preferred_element_type=wide
        )
        error = error - tgt[0:half, cols]
        m = masked[:, cols]
        sc = m * error
        scored[:, cols] = sc
        sc_low[0:half, cols] = sc.astype(low)
        esum = jnp.sum(sc * error, axis=0, keepdims=True)
        wsum = jnp.sum(m, axis=0, keepdims=True)
        for n in range(2):
            r = side * 2 + n
            msg[r : r + 1, :] = esum[:, n * TILE : (n + 1) * TILE]
            msg[4 + r : 5 + r, :] = wsum[:, n * TILE : (n + 1) * TILE]

    def share(src, slots, me, peers, base):
        copies = [remote(src, slots.at[me], tsend, trecv, base + n, peer) for n, peer in enumerate(peers)]
        slots[me] = src[...]
        return copies

    first_share = share(msg, near, mine, [near_peer(d) for d in range(1, 8)], 0)

    def scored_cols(side, c):
        return pl.ds(pl.multiple_of(side * vw + c * TILE, TILE), TILE)

    score_copies = [
        remote(sc_low.at[:, scored_cols(n, oc)], sc_par.at[:, pl.ds(n * TILE, TILE)], dsend, drecv, n, partner)
        for n in range(2)
    ]
    flips = [flip_to(h_two, t_two, 2), flip_to(h_one, t_one, 3)] + flips
    make_slope(pre_two)
    for copy in first_share:
        copy.wait_recv()
    mid[...] = jnp.sum(near[...], axis=0)
    second_share = share(mid, far, high, [far_peer(d) for d in range(1, 4)], 7)

    mark_bits = {"z": zn, "y": yy}

    def produce(g, trans, own_cols, par_cols):
        first = PLAN[g][0]
        value = mark_bits[first]
        both_cols = jnp.concatenate([own_cols, par_cols], axis=0)

        def product(v):
            def side_rows(k):
                blocks = []
                for i in range(2):
                    for j in range(2):
                        index = i * 4 + (j * 2 + v if first == "y" else v * 2 + j)
                        blocks.append(trans[k, at(index, TILE), :])
                return jnp.concatenate(blocks, axis=0)

            both_rows = jnp.concatenate([side_rows(0), side_rows(1)], axis=1)
            out = jnp.dot(both_rows, both_cols, preferred_element_type=wide)
            return out.reshape(2, 2, TILE, vw)

        fars[g][0][...] = product(1 - value).astype(low)
        copy = remote(fars[g][0], arrs[g][0], rsend, rrecv, 6 * g, (flipped(s, BITS[first]), x))
        nears[g][0][...] = product(value)
        return copy

    def advance(g, n, copy):
        copy.wait_recv()
        way = PLAN[g][n]
        ref, came = nears[g][n - 1], arrs[g][n - 1]
        if way == "x":
            lead = (slice(None),) * (len(ref.shape) - 1)
            away, here, target = lead + (at(other, TILE),), lead + (at(x, TILE),), across
        else:
            value = mark_bits[way]
            away, here = (slice(None), 1 - value), (slice(None), value)
            target = (flipped(s, BITS[way]), x)
        fars[g][n][...] = (ref[away] + came[away].astype(wide)).astype(low)
        copy = remote(fars[g][n], arrs[g][n], rsend, rrecv, 6 * g + n, target)
        nears[g][n][...] = ref[here] + came[here].astype(wide)
        return copy

    def advance_last(g, copy):
        copy.wait_recv()
        ref, came = nears[g][2], arrs[g][2]
        finals[g] = (ref[1 - zf] + came[1 - zf].astype(wide)).astype(low)
        up = (flipped(s, 3), x)
        copies = [
            remote(finals.at[g, at(core, hr), :], arrs4.at[g], rsend, rrecv, 6 * g + 3, up),
            remote(finals.at[g, at(oc, hr), :], arrs5.at[g], rsend, rrecv, 6 * g + 4, diagonal),
        ]
        ref[zf] = ref[zf] + came[zf].astype(wide)
        copies.append(remote(ref.at[zf, at(oc, hr), :], arrs3.at[g], rsend, rrecv, 6 * g + 5, partner))
        return copies

    def finish(g, copies, out, base):
        for copy in copies:
            copy.wait_recv()
        kept = nears[g][2][zf, at(core, hr), :] + arrs4[g].astype(wide)
        came = arrs3[g] + arrs5[g].astype(wide)
        span = out.shape[1] // 2
        out[pl.ds(0, hr), pl.ds(pl.multiple_of(core * span + base, TILE), TILE)] = kept
        out[pl.ds(0, hr), pl.ds(pl.multiple_of(oc * span + base, TILE), TILE)] = came

    for copy in score_copies:
        copy.wait_recv()
    flips[0].wait_recv()
    state = {}
    own = jnp.concatenate([sc_low[:, scored_cols(n, core)] for n in range(2)], axis=1)
    state[0] = produce(0, t_two, own, sc_par[...])
    make_slope(pre_one)
    for copy in second_share:
        copy.wait_recv()
    sums = jnp.sum(far[...], axis=0)
    tl = lax.broadcasted_iota(jnp.int32, (8, TILE), 1)
    sums = sums + jnp.where(tl % 2 == 0, pltpu.roll(sums, TILE - 1, 1), pltpu.roll(sums, 1, 1))
    sums = sums + jnp.where(tl % 4 < 2, pltpu.roll(sums, TILE - 2, 1), pltpu.roll(sums, 2, 1))
    kinds = 2 * rows // PP
    line = lax.broadcasted_iota(jnp.int32, (4, TILE), 0)
    tl = lax.broadcasted_iota(jnp.int32, (4, TILE), 1)
    ok = (line % 2) * TILE + tl < rows
    weight_sum = jnp.where(ok, sums[4:8, :], 1.0)
    root = jnp.sqrt(jnp.where(ok, sums[0:4, :], 0.0) / weight_sum + 1e-06)
    roots = jnp.where(ok & (tl % PP == 0), root, 0.0)
    loss = jnp.sum(jnp.sum(roots, axis=0, keepdims=True), axis=1, keepdims=True) / kinds
    r_loss[...] = jnp.broadcast_to(loss, r_loss.shape)
    write_out(r_loss, o_loss)
    coef = jnp.where(ok, scale[0] / (kinds * root * weight_sum), 0.0)
    coef = jnp.concatenate([coef[n : n + 1, :] for n in range(4)], axis=1)
    gp_low[...] = (coef * scored[...]).astype(low)

    def grad_tiles(made, send_to, base, make):
        for n in range(dim // vw):
            tile = pl.ds(n * vw, vw)
            made[0:half, tile] = make(tile)
        return [
            remote(
                made.at[:, pl.ds(pl.multiple_of(side * width + oc * vw, vw), vw)],
                send_to.at[:, pl.ds(side * vw, vw)],
                dsend, drecv, base + side, partner,
            )
            for side in range(2)
        ]

    def make_two(tile):
        b = jnp.dot(gp_low[...], w_head[:, tile], preferred_element_type=wide)
        return (b * pre_two[:, tile]).astype(low)

    two_copies = grad_tiles(g_two, p_two, 5, make_two)

    def make_one(tile):
        b = lax.dot_general(
            g_two[0:half, :], w_two[tile, :], (((1,), (1,)), ((), ())), preferred_element_type=wide
        )
        return (b * pre_one[:, tile]).astype(low)

    one_copies = grad_tiles(g_one, p_one, 7, make_one)

    def both(made, came, a):
        own_cols = [
            made[:, pl.ds(pl.multiple_of(n * width + core * vw + a * TILE, TILE), TILE)] for n in range(2)
        ]
        par_cols = [came[:, n * vw + a * TILE : n * vw + (a + 1) * TILE] for n in range(2)]
        return jnp.concatenate(own_cols, axis=1), jnp.concatenate(par_cols, axis=1)

    def token_side(side, out):
        for n in range(width // vw):
            b = lax.dot_general(
                g_one[0:half, :],
                w_one[pl.ds(pl.multiple_of(side * width + n * vw, vw), vw), :],
                (((1,), (1,)), ((), ())),
                preferred_element_type=wide,
            )
            out[:, n * vw : (n + 1) * vw] = b.astype(low)

    for copy in two_copies + [flips[1]]:
        copy.wait_recv()
    for a in range(2):
        state[1 + a] = produce(1 + a, t_one, *both(g_two, p_two, a))
    token_side(other, tg_far)
    state[0] = advance(0, 1, state[0])
    tg_copy = remote(tg_far, o_tok.at[at(x, half), :], xsend, xrecv, parts + 1, across)
    for copy in one_copies + [flips[2]]:
        copy.wait_recv()
    for a in range(2):
        state[3 + a] = produce(3 + a, t_tok, *both(g_one, p_one, a))
    token_side(x, tg_near)
    write_out(tg_near, o_tok.at[at(x, half), :])
    state[0] = advance(0, 2, state[0])
    state[1] = advance(1, 1, state[1])
    state[2] = advance(2, 1, state[2])
    state[3] = advance(3, 1, state[3])
    state[4] = advance(4, 1, state[4])
    state[0] = advance_last(0, state[0])
    state[2] = advance(2, 2, state[2])
    state[1] = advance(1, 2, state[1])
    state[3] = advance(3, 2, state[3])
    state[4] = advance(4, 2, state[4])
    finish(0, state[0], hb, 0)
    coef_here = jnp.where(x == 0, coef[:, :vw], coef[:, vw:])
    r_head[...] = (hb[...] * coef_here)[:, 0:rows]
    write_out(r_head, o_head)
    state[2] = advance_last(2, state[2])
    state[1] = advance_last(1, state[1])
    state[3] = advance_last(3, state[3])
    state[4] = advance_last(4, state[4])
    finish(2, state[2], r_two, TILE)
    finish(1, state[1], r_two, 0)
    write_out(r_two, o_two)
    finish(3, state[3], r_one, 0)
    finish(4, state[4], r_one, TILE)
    write_out(r_one, o_one)
    tg_copy.wait_recv()
    for copy in started:
        copy.wait_send()
    for copy in writes:
        copy.wait()


def fused(scale, kinds, land, tokens, first, second, head, targets):
    count, width = tokens.shape
    dim = first.shape[0]
    rows = head.shape[0]
    half = count // 2
    pad = -(-half // TILE) * TILE
    vw = 2 * TILE
    hr = TILE // 2
    low, wide = jnp.bfloat16, jnp.float32
    shape = jax.ShapeDtypeStruct
    slices = len(PLAN)
    vm = pltpu.VMEM
    scratch = [
        vm((dim, dim), low), vm((dim, dim), low), vm((2 * vw, dim), low), vm((pad, dim), low),
        vm((half, width), low), vm((rows, count), wide), vm((rows, pad), low), vm((2, vw, pad), low),
        vm((TILE, count), wide), vm((half, 2 * vw), wide),
        vm((half, dim), wide), vm((half, dim), wide), vm((pad, dim), low), vm((pad, dim), low),
        vm((2, dim, pad), low), vm((2, dim, pad), low), vm((2, dim, pad), low),
        vm((pad, 2 * vw), wide), vm((half, 2 * vw), wide), vm((pad, 2 * vw), low), vm((pad, vw), low),
        vm((half, 2 * vw), low),
        vm((pad, dim), low), vm((pad, dim), low), vm((pad, width), low), vm((pad, width), low),
        vm((half, width), low), vm((half, width), low),
        vm((hr, width), wide), vm((hr, width), wide), vm((hr, rows), wide), vm((hr, vw), wide),
        vm((8, TILE), wide), vm((8, TILE), wide), vm((8, TILE), wide),
        vm((8, TILE), wide), vm((8, 8, TILE), wide), vm((4, 8, TILE), wide), vm((8, TILE), wide),
        vm((slices, TILE, TILE), low), vm((slices, hr, TILE), wide),
        vm((slices, hr, TILE), low), vm((slices, hr, TILE), low),
    ]
    for kind in (low, low, wide):
        for order in PLAN:
            scratch += [vm(found, kind) for found in stage_shapes(order)]
    sizes = (6, 48, 48, 5, 5, 9, 9, 10, 10, 6 * slices, 6 * slices, 5)
    scratch += [pltpu.SemaphoreType.DMA((n,)) for n in sizes]
    return pl.pallas_call(
        fused_kernel,
        out_shape=(
            shape((8, TILE), wide),
            shape((count, width), low),
            shape((dim // 16, width), wide),
            shape((dim // 16, width), wide),
            shape((hr, rows), wide),
        ),
        in_specs=[pl.BlockSpec(memory_space=pltpu.SMEM), VMEM, VMEM] + [ANY] * 5,
        out_specs=[ANY] * 5,
        scratch_shapes=scratch,
        compiler_params=params(0, 56),
        name="fused",
    )(scale, kinds, land, tokens, first, second, head, targets)


CHUNKS = 4


def write_kernel(
    loss, tok, one, two, head, o_loss, o_tok, o_one, o_two, o_head,
    v_loss, v_tok, v_one, v_two, v_head, f_loss, f_tok, came, went,
):
    size = tok.shape[0] // CHUNKS
    loads = [
        pltpu.make_async_copy(tok.at[pl.ds(n * size, size), :], v_tok.at[pl.ds(n * size, size), :], came.at[n])
        for n in range(CHUNKS)
    ]
    small = [(one, v_one, o_one), (two, v_two, o_two), (head, v_head, o_head), (loss, v_loss, None)]
    loads += [pltpu.make_async_copy(a, b, came.at[CHUNKS + n]) for n, (a, b, _) in enumerate(small)]
    for copy in loads:
        copy.start()
    stores = []

    def store(src, dst):
        copy = pltpu.make_async_copy(src, dst, went.at[len(stores)])
        copy.start()
        stores.append(copy)

    for n in range(CHUNKS):
        loads[n].wait()
        span = pl.ds(n * size, size)
        f_tok[span, :] = v_tok[span, :].astype(jnp.float32)
        store(f_tok.at[span, :], o_tok.at[span, :])
    for n, (_, b, c) in enumerate(small):
        loads[CHUNKS + n].wait()
        if c is None:
            f_loss[...] = b[0:1, 0:1]
            b, c = f_loss, o_loss
        store(b, c)
    for copy in stores:
        copy.wait()


def write(*parts):
    wide = jnp.float32
    shapes = [(1, 1)] + [p.shape for p in parts[1:]]
    vm = pltpu.VMEM
    return pl.pallas_call(
        write_kernel,
        out_shape=tuple(jax.ShapeDtypeStruct(a, wide) for a in shapes),
        in_specs=[ANY] * 5,
        out_specs=[ANY] * 5,
        scratch_shapes=[vm(p.shape, p.dtype) for p in parts]
        + [vm((1, 1), wide), vm(parts[1].shape, wide)]
        + [pltpu.SemaphoreType.DMA((CHUNKS + 4,)), pltpu.SemaphoreType.DMA((CHUNKS + 4,))],
        name="write",
    )(*parts)


def per_device(
    tokens, first_weight, second_weight, head_weight, targets, land_mask, variable_kind, loss_scale
):
    parts = fused(
        loss_scale.reshape(1), variable_kind.reshape(1, -1), land_mask,
        tokens, first_weight, second_weight, head_weight, targets,
    )
    loss, token_grad, first_grad, second_grad, head_grad = write(*parts)
    return (loss.reshape(()), token_grad, first_grad, second_grad, head_grad.T)


def column_folder(weights, piece):
    return lax.dot_general(
        piece, weights, (((1,), (1,)), ((), ())), preferred_element_type=jnp.float32
    )


def row_folder(weights, piece):
    return lax.dot_general(
        piece, weights, (((0,), (0,)), ((), ())), preferred_element_type=jnp.float32
    )


def per_device_wide(
    tokens, first_weight, second_weight, head_weight, targets, land_mask, variable_kind, loss_scale
):
    count = tokens.shape[0]
    width = first_weight.shape[1]
    kinds = head_weight.shape[0] // PP
    rows_first, rows_second = (
        lax.all_to_all(first_weight, "tensor", split_axis=0, concat_axis=1, tiled=True),
        lax.all_to_all(second_weight, "tensor", split_axis=0, concat_axis=1, tiled=True),
    )
    head_cols = lax.all_to_all(head_weight, "tensor", split_axis=1, concat_axis=0, tiled=True)
    position = lax.axis_index("space") * count + jnp.arange(count, dtype=jnp.int32)
    cell = jnp.arange(PP, dtype=jnp.int32)
    lat_row = 2 * (position // LONP)[None, :] + (cell // 2)[:, None]
    nlat = 2 * PROW_DEV * lax.axis_size("space")
    cell_weight = jnp.cos(math.pi / 2.0 * (lat_row.astype(jnp.float32) + 0.5) / nlat)
    land = land_mask.astype(jnp.float32)
    kind = variable_kind[:, None, None]
    valid = jnp.where(kind == 0, 1.0, jnp.where(kind == 1, land[None], 1.0 - land[None]))
    masked = cell_weight[None] * valid
    local_weight = jnp.sum(masked, axis=(1, 2))
    weight_sum = lax.psum(local_weight, "space")
    full_in = lax.all_gather(tokens, "tensor", axis=1, tiled=True)
    pre_one = jnp.dot(full_in, first_weight, preferred_element_type=jnp.float32)
    hidden_one = jax.nn.gelu(pre_one, approximate=False).astype(jnp.bfloat16)
    full_one = lax.all_gather(hidden_one, "tensor", axis=1, tiled=True)
    pre_two = jnp.dot(full_one, second_weight, preferred_element_type=jnp.float32)
    hidden_two = jax.nn.gelu(pre_two, approximate=False).astype(jnp.bfloat16)
    full_two = lax.all_gather(hidden_two, "tensor", axis=1, tiled=True)
    predicted = lax.dot_general(
        head_weight, full_two, (((1,), (1,)), ((), ())), preferred_element_type=jnp.float32
    )
    error = predicted.reshape(kinds, PP, count) - targets.reshape(kinds, PP, count)
    local_error = jnp.sum(masked * error * error, axis=(1, 2))
    error_sum = lax.psum(local_error, "space")
    root = jnp.sqrt(error_sum / weight_sum + 1e-06)
    loss = lax.psum(jnp.sum(root), "tensor") / (kinds * lax.axis_size("tensor"))
    coef = loss_scale / (kinds * lax.axis_size("tensor") * root * weight_sum)
    grad_pred = (
        (coef[:, None, None] * masked * error).reshape(kinds * PP, count).astype(jnp.bfloat16)
    )
    back_two = row_folder(head_cols, lax.all_gather(grad_pred, "tensor", axis=0, tiled=True))
    head_term = jnp.dot(grad_pred, full_two, preferred_element_type=jnp.float32)
    head_grad = lax.psum_scatter(head_term, "space", scatter_dimension=1, tiled=True)
    grad_two = (back_two * slope(pre_two)).astype(jnp.bfloat16)
    back_one = column_folder(rows_second, lax.all_gather(grad_two, "tensor", axis=1, tiled=True))
    grad_one = (back_one * slope(pre_one)).astype(jnp.bfloat16)
    joined = lax.psum_scatter(
        jnp.concatenate(
            [
                lax.dot_general(
                    full_one, grad_two, (((0,), (0,)), ((), ())), preferred_element_type=jnp.float32
                ),
                lax.dot_general(
                    full_in, grad_one, (((0,), (0,)), ((), ())), preferred_element_type=jnp.float32
                ),
            ],
            axis=1,
        ),
        "space",
        scatter_dimension=0,
        tiled=True,
    )
    second_grad = joined[:, :width]
    first_grad = joined[:, width:]
    token_grad = column_folder(rows_first, lax.all_gather(grad_one, "tensor", axis=1, tiled=True))
    return (loss, token_grad, first_grad, second_grad, head_grad)


def solution(mesh):
    size = mesh.shape["space"]
    paired = mesh.shape["tensor"] == 2 and size == 16
    return jax.shard_map(
        per_device if paired else per_device_wide,
        mesh=mesh,
        in_specs=(
            P("space", "tensor"),
            P(None, "tensor"),
            P(None, "tensor"),
            P("tensor", None),
            P("tensor", "space"),
            P(None, "space"),
            P("tensor"),
            P(),
        ),
        out_specs=(
            P(),
            P("space", "tensor"),
            P("space", "tensor"),
            P("space", "tensor"),
            P("tensor", "space"),
        ),
        check_vma=False,
    )
```

```python
import math

import jax
import jax.numpy as jnp
from jax import lax
from jax.experimental import pallas as pl
from jax.experimental.pallas import tpu as pltpu
from jax.sharding import PartitionSpec as P

PP = 4
PROW_DEV = 4
LONP = 224
MESH = pl.DeviceIdType.MESH
VMEM = pl.BlockSpec(memory_space=pltpu.VMEM)
ANY = pl.BlockSpec(memory_space=pl.ANY)


def bent(z):
    return (0.5 * z * (1.0 + lax.erf(z / math.sqrt(2.0)))).astype(jnp.bfloat16)


def slope(z):
    cdf = 0.5 * (1.0 + lax.erf(z / math.sqrt(2.0)))
    return cdf + z * jnp.exp(-0.5 * z * z) / math.sqrt(2.0 * math.pi)


def flipped(s, bit):
    step = 1 << bit
    return s + step - 2 * step * ((s // step) % 2)


def greet(partners):
    barrier = pltpu.get_barrier_semaphore()
    for partner in partners:
        pl.semaphore_signal(barrier, inc=1, device_id=partner, device_id_type=MESH)
    pl.semaphore_wait(barrier, len(partners))


def params(number, mib):
    return pltpu.CompilerParams(
        collective_id=number, has_side_effects=True, vmem_limit_bytes=mib * 2**20
    )


HBM = pl.BlockSpec(memory_space=pltpu.HBM)
TILE = 128
TREES = ((2, 1, 0), (3, 2, 1, 0), (1, 3, 2, 0))
SLICES = 5
BITS = {"z": 2, "y": 1}
PLAN = {
    (0, 0): "yzx", (0, 1): "yxz", (1, 0): "zyx", (1, 1): "yxz", (2, 0): "yzx", (2, 1): "zyx", (3, 0): "zyx",
    (3, 1): "yxz", (4, 0): "zxy", (4, 1): "yzx",
}
STEPS = (
    "C", "A001", "T1", "P20", "P21", "T0", "P40", "P41", "A011", "P10", "P11", "A002", "P31", "N", "P30",
    "A201", "A211", "A411", "A401", "A111", "A101", "A012", "A311", "A301", "A402", "A212", "A202", "A112",
    "A102", "A412", "A312", "L0", "A302", "L2", "L1", "L4", "L3", "F0", "F2", "F1", "F4", "F3",
)


def stage_shapes(order):
    found = []
    left, lanes = 3, 2 * TILE
    for way in order:
        if way == "x":
            lanes = TILE
        else:
            left -= 1
        found.append((2,) * left + (TILE // 2, lanes))
    return found


def fused_kernel(
    scale, kinds_in, land, tok, one, two, head, tar,
    o_loss, o_tok, o_one, o_two, o_head,
    w_one, w_two, w_head, toks, tok_out, tar_v, tar_s, tar_all, lnd, masked,
    pre_one, pre_two, h_one, h_two, t_tok, t_one, t_two, tgt, scored, sc_low, sc_par, gp_low,
    g_two, g_one, p_two, p_one, tg_far, hb, kb, kp,
    msg, near, far, mid, finals, arrs3, arrs4, arrs5, *refs,
):
    keys = sorted(PLAN)
    pick_refs = iter(refs)
    fars, arrs, nears = [{key: [next(pick_refs), next(pick_refs)] for key in keys} for _ in range(3)]
    fars2, arrs2, nears2 = [next(pick_refs) for _ in range(3)]
    for store, final in ((fars, fars2), (arrs, arrs2), (nears, nears2)):
        for g, h in keys:
            store[g, h].append(final.at[g, h])
    local, wsend, wrecv, xsend, xrecv, dsend, drecv, tsend, trecv, rsend, rrecv = pick_refs
    low, wide = jnp.bfloat16, jnp.float32
    s, x = lax.axis_index("space"), lax.axis_index("tensor")
    other = 1 - x
    zf, zn, yy, core = (s // 8) % 2, (s // 4) % 2, (s // 2) % 2, s % 2
    oc = 1 - core
    count = tok.shape[0]
    half = count // 2
    dim, width = one.shape
    rows = head.shape[0]
    pad = toks.shape[0]
    vw = 2 * TILE
    hr = TILE // 2
    across, partner = (s, other), (flipped(s, 0), x)
    diagonal = (flipped(flipped(s, 3), 0), x)
    started = []

    def at(index, size):
        return pl.ds(pl.multiple_of(index * size, size), size)

    def remote(src, dst, sends, recvs, slot, target):
        copy = pltpu.make_async_remote_copy(
            src_ref=src,
            dst_ref=dst,
            send_sem=sends.at[slot],
            recv_sem=recvs.at[slot],
            device_id=target,
            device_id_type=MESH,
        )
        copy.start()
        started.append(copy)
        return copy

    moves = [
        (one, w_one.at[:, at(x, width)]),
        (two, w_two.at[:, at(x, width)]),
        (head, w_head.at[pl.ds(pl.multiple_of(x * vw, vw), rows), :]),
        (tok.at[at(other, half), :], tok_out),
        (tar, tar_v),
        (tok.at[at(x, half), :], toks.at[pl.ds(0, half), at(x, width)]),
    ]
    loads = [pltpu.make_async_copy(a, b, local.at[n]) for n, (a, b) in enumerate(moves)]
    for copy in loads:
        copy.start()

    shard = 96
    w_head[pl.ds(pl.multiple_of(x * vw + rows, 16), vw - rows), :] = jnp.zeros((vw - rows, dim), low)
    w_head[pl.ds(pl.multiple_of(other * vw + 2 * shard, 16), vw - 2 * shard), :] = jnp.zeros(
        (vw - 2 * shard, dim), low
    )
    for ref in (toks, h_one, h_two, g_two, g_one, sc_low):
        ref[half:, :] = jnp.zeros((pad - half, ref.shape[1]), low)
    tar_all[:, rows:, :] = jnp.zeros((2, vw - rows, pad), low)
    kb[...] = jnp.zeros_like(kb)
    kb[0:1, 0 : rows // PP] = kinds_in[...].astype(wide)
    lnd[...] = jnp.zeros_like(lnd)
    lnd[0:PP, :] = land[...].astype(wide)

    low_bits, high = s % 4, s // 4
    mine = x * 4 + low_bits

    def near_peer(d):
        j = (mine + d) % 8
        return (high * 4 + j % 4, j // 4)

    def far_peer(d):
        return (((high + d) % 4) * 4 + low_bits, x)

    greet([near_peer(d) for d in range(1, 8)] + [far_peer(d) for d in range(1, 4)] + [diagonal])

    part = dim // 16

    def place(k, m, side):
        q = s
        for b in range(4):
            if (m >> b) & 1:
                q = flipped(q, b)
        if k == 0:
            return w_one.at[at(q % 8, 2 * part), at(side, width)]
        if k == 1:
            return w_two.at[at(q, part), at(side, width)]
        first = pl.multiple_of(side * vw + (q % 2) * shard, 16)
        return w_head.at[pl.ds(first, shard), at(q // 2, TILE)]

    pieces = {}
    for k in range(3):
        loads[k].wait()
        pieces[k, 0] = remote(place(k, 0, x), place(k, 0, x), wsend, wrecv, 16 * k, across)
    kind_copy = remote(kb, kp, xsend, xrecv, 4, across)
    loads[3].wait()
    parts = 2
    step = half // parts
    tok_copies = [
        remote(
            tok_out.at[pl.ds(n * step, step), :],
            toks.at[pl.ds(n * step, step), at(x, width)],
            xsend, xrecv, n, across,
        )
        for n in range(parts)
    ]
    loads[4].wait()
    tail = count - pad
    lo = tar_v[:, :pad]
    hi = pltpu.roll(tar_v[:, tail:], pad - half + tail, 1)
    tar_s[...] = jnp.where(x == 0, hi, lo).astype(low)
    tar_copy = remote(tar_s, tar_all.at[x, pl.ds(0, rows), :], xsend, xrecv, parts, across)
    tar_all[x, 0:rows, :] = jnp.where(x == 0, lo, hi).astype(low)
    loads[5].wait()

    def relay(k, *ms):
        for m in ms:
            pieces[k, m].wait_recv()
            last = -1
            for n, b in enumerate(TREES[k]):
                if (m >> b) & 1:
                    last = n
            for b in TREES[k][last + 1 :]:
                piece = place(k, m, other)
                new = m ^ (1 << b)
                pieces[k, new] = remote(piece, piece, wsend, wrecv, 16 * k + new, (flipped(s, b), x))

    def layer(src, first, size, weight, side, pre, dst):
        span = slice(first, first + size)
        for i in range(width // vw):
            tile = pl.ds(pl.multiple_of(side * width + i * vw, vw), vw)
            z = jnp.dot(src[span, :], weight[:, tile], preferred_element_type=wide)
            pre[span, tile] = z
            dst[span, tile] = bent(z)

    def flip_to(src, dst, slot):
        for n in range(dim // TILE):
            dst[0, n * TILE : (n + 1) * TILE, :] = src[:, n * TILE : (n + 1) * TILE].T
        return remote(dst.at[0], dst.at[1], dsend, drecv, slot, partner)

    def make_slope(ref):
        def body(n, _):
            ref[:, at(n, TILE)] = slope(ref[:, at(n, TILE)])
            return 0

        lax.fori_loop(0, dim // TILE, body, 0)

    relay(0, 0)
    relay(1, 0)
    relay(2, 0)
    kind_copy.wait_recv()
    lane = lax.broadcasted_iota(jnp.int32, (1, 2 * vw), 1)
    used = lane % vw < rows
    cell = lane % PP
    group_shape = (TILE, vw)
    group = lax.broadcasted_iota(jnp.int32, group_shape, 1) // PP == lax.broadcasted_iota(jnp.int32, group_shape, 0)
    group = jnp.where(group, 1.0, 0.0).astype(low)
    k_own = jnp.dot(kb[...].astype(low), group, preferred_element_type=wide)[0:1, :]
    k_oth = jnp.dot(kp[...].astype(low), group, preferred_element_type=wide)[0:1, :]
    kind = jnp.concatenate([jnp.where(x == 0, k_own, k_oth), jnp.where(x == 0, k_oth, k_own)], axis=1)
    ground = jnp.where(x == 0, lnd[:, :pad], pltpu.roll(lnd[:, tail:], pad - half + tail, 1))
    pick_shape = (TILE, 2 * vw)
    pick = lax.broadcasted_iota(jnp.int32, pick_shape, 1) % PP == lax.broadcasted_iota(jnp.int32, pick_shape, 0)
    spread = jnp.dot(
        ground.T.astype(low), jnp.where(pick, 1.0, 0.0).astype(low), preferred_element_type=wide
    )
    bands = half // LONP
    nlat = 2 * (count // LONP) * lax.axis_size("space")
    for j in range(bands):
        lat_row = 2 * (s * (count // LONP) + x * bands + j) + cell // 2
        weight = jnp.cos(math.pi / 2.0 * (lat_row.astype(wide) + 0.5) / nlat)
        weight = jnp.where(used, weight, 0.0)
        flat = jnp.where(kind == 1.0, 0.0, weight)
        slant = jnp.where(kind == 1.0, weight, jnp.where(kind == 2.0, -weight, 0.0))
        band = slice(j * LONP, (j + 1) * LONP)
        masked[band, :] = flat + slant * spread[band, :]
    relay(0, 4, 2)
    relay(1, 2, 4)
    relay(2, 2)
    relay(1, 8)
    tgt[:, at(x, vw)] = tar_all[x].astype(wide).T
    relay(2, 4, 8)
    tok_copies[0].wait_recv()
    layer(toks, 0, step, w_one, x, pre_one, h_one)
    relay(0, 6)
    relay(1, 12)
    relay(2, 6)
    relay(0, 1, 5, 3, 7)
    layer(toks, 0, step, w_one, other, pre_one, h_one)
    relay(1, 6)
    relay(2, 10, 12)
    tok_copies[1].wait_recv()
    layer(toks, step, half - step, w_one, x, pre_one, h_one)
    layer(toks, step, half - step, w_one, other, pre_one, h_one)
    relay(1, 10, 14)
    layer(h_one, 0, half, w_two, x, pre_two, h_two)
    relay(2, 14)
    relay(1, 1, 9, 5, 13, 3, 11, 7, 15)
    layer(h_one, 0, half, w_two, other, pre_two, h_two)
    relay(2, 1, 9, 5, 13, 3, 11, 7, 15)
    tar_copy.wait_recv()
    tgt[:, at(other, vw)] = tar_all[other].astype(wide).T
    for side in range(2):
        cols = slice(side * vw, (side + 1) * vw)
        error = lax.dot_general(
            h_two[0:half, :], w_head[cols, :], (((1,), (1,)), ((), ())), preferred_element_type=wide
        )
        error = error - tgt[0:half, cols]
        m = masked[:, cols]
        sc = m * error
        scored[:, cols] = sc
        sc_low[0:half, cols] = sc.astype(low)
        esum = jnp.sum(sc * error, axis=0, keepdims=True)
        wsum = jnp.sum(m, axis=0, keepdims=True)
        for n in range(2):
            r = side * 2 + n
            msg[r : r + 1, :] = esum[:, n * TILE : (n + 1) * TILE]
            msg[4 + r : 5 + r, :] = wsum[:, n * TILE : (n + 1) * TILE]

    def share(src, slots, me, peers, base):
        copies = [remote(src, slots.at[me], tsend, trecv, base + n, peer) for n, peer in enumerate(peers)]
        slots[me] = src[...]
        return copies

    first_share = share(msg, near, mine, [near_peer(d) for d in range(1, 8)], 0)

    def scored_cols(side, c):
        return pl.ds(pl.multiple_of(side * vw + c * TILE, TILE), TILE)

    score_copies = [
        remote(sc_low.at[:, scored_cols(n, oc)], sc_par.at[:, pl.ds(n * TILE, TILE)], dsend, drecv, n, partner)
        for n in range(2)
    ]
    flips = [flip_to(h_two, t_two, 2), flip_to(h_one, t_one, 3), flip_to(toks, t_tok, 4)]
    make_slope(pre_two)
    for copy in first_share:
        copy.wait_recv()
    mid[...] = jnp.sum(near[...], axis=0)
    second_share = share(mid, far, high, [far_peer(d) for d in range(1, 4)], 7)

    mark_bits = {"z": zn, "y": yy}

    def goal(way):
        return across if way == "x" else (flipped(s, BITS[way]), x)

    def produce(g, h, trans, own_cols, par_cols):
        first = PLAN[g, h][0]
        both_cols = jnp.concatenate([own_cols, par_cols], axis=0)
        ref, store = fars[g, h][0], nears[g, h][0]

        def product(blocks):
            sides = [
                jnp.concatenate(
                    [trans[k, pl.ds(pl.multiple_of(b * TILE + h * hr, hr), hr), :] for b in blocks], axis=0
                )
                for k in range(2)
            ]
            return jnp.dot(jnp.concatenate(sides, axis=1), both_cols, preferred_element_type=wide)

        def blocks_of(v):
            return [i * 4 + (j * 2 + v if first == "y" else v * 2 + j) for i in range(2) for j in range(2)]

        if first == "x":
            out = product(list(range(8)))
            ref[...] = jnp.where(x == 0, out[:, TILE:], out[:, :TILE]).astype(low).reshape(ref.shape)
            store[...] = jnp.where(x == 0, out[:, :TILE], out[:, TILE:]).reshape(ref.shape)
        else:
            value = mark_bits[first]
            out = product(blocks_of(1 - value) + blocks_of(value))
            ref[...] = out[: 4 * hr].astype(low).reshape(ref.shape)
        copy = remote(ref, arrs[g, h][0], rsend, rrecv, 9 * g + 3 * h, goal(first))
        if first != "x":
            store[...] = out[4 * hr :].reshape(ref.shape)
        return copy

    def advance(g, h, n, copy):
        copy.wait_recv()
        order = PLAN[g, h]
        way = order[n]
        left = [d for d in "fzy" if d not in order[:n]]
        ref, came = nears[g, h][n - 1], arrs[g, h][n - 1]
        if way == "x":
            lead = (slice(None),) * (len(left) + 1)
            away, here = lead + (at(other, TILE),), lead + (at(x, TILE),)
        else:
            lead = (slice(None),) * left.index(way)
            away, here = lead + (1 - mark_bits[way],), lead + (mark_bits[way],)
        fars[g, h][n][...] = (ref[away] + came[away].astype(wide)).astype(low)
        copy = remote(fars[g, h][n], arrs[g, h][n], rsend, rrecv, 9 * g + 3 * h + n, goal(way))
        nears[g, h][n][...] = ref[here] + came[here].astype(wide)
        return copy

    def advance_last(g, before):
        for h in range(2):
            before[h].wait_recv()
            finals[g, h] = (nears2[g, h, 1 - zf] + arrs2[g, h, 1 - zf].astype(wide)).astype(low)
        up = (flipped(s, 3), x)
        copies = [
            remote(finals.at[g, core], arrs4.at[g], rsend, rrecv, 9 * g + 6, up),
            remote(finals.at[g, oc], arrs5.at[g], rsend, rrecv, 9 * g + 7, diagonal),
        ]
        for h in range(2):
            nears2[g, h, zf] = nears2[g, h, zf] + arrs2[g, h, zf].astype(wide)
        copies.append(remote(nears2.at[g, oc, zf], arrs3.at[g], rsend, rrecv, 9 * g + 8, partner))
        return copies

    def finish(g, copies, out, base):
        for copy in copies:
            copy.wait_recv()
        kept = nears2[g, core, zf] + arrs4[g].astype(wide)
        came = arrs3[g] + arrs5[g].astype(wide)
        span = out.shape[1] // 2
        out[pl.ds(0, hr), pl.ds(pl.multiple_of(core * span + base, TILE), TILE)] = kept
        out[pl.ds(0, hr), pl.ds(pl.multiple_of(oc * span + base, TILE), TILE)] = came

    for copy in score_copies:
        copy.wait_recv()
    flips[0].wait_recv()
    state = {}
    own = jnp.concatenate([sc_low[:, scored_cols(n, core)] for n in range(2)], axis=1)
    for h in range(2):
        state[0, h] = produce(0, h, t_two, own, sc_par[...])
    make_slope(pre_one)
    for copy in second_share:
        copy.wait_recv()
    sums = jnp.sum(far[...], axis=0)
    tl = lax.broadcasted_iota(jnp.int32, (8, TILE), 1)
    sums = sums + jnp.where(tl % 2 == 0, pltpu.roll(sums, TILE - 1, 1), pltpu.roll(sums, 1, 1))
    sums = sums + jnp.where(tl % 4 < 2, pltpu.roll(sums, TILE - 2, 1), pltpu.roll(sums, 2, 1))
    kinds = 2 * rows // PP
    line = lax.broadcasted_iota(jnp.int32, (4, TILE), 0)
    tl = lax.broadcasted_iota(jnp.int32, (4, TILE), 1)
    ok = (line % 2) * TILE + tl < rows
    weight_sum = jnp.where(ok, sums[4:8, :], 1.0)
    root = jnp.sqrt(jnp.where(ok, sums[0:4, :], 0.0) / weight_sum + 1e-06)
    roots = jnp.where(ok & (tl % PP == 0), root, 0.0)
    loss = jnp.sum(jnp.sum(roots, axis=0, keepdims=True), axis=1, keepdims=True) / kinds
    o_loss[...] = jnp.broadcast_to(loss, o_loss.shape)
    coef = jnp.where(ok, scale[0] / (kinds * root * weight_sum), 0.0)
    coef = jnp.concatenate([coef[n : n + 1, :] for n in range(4)], axis=1)
    gp_low[...] = (coef * scored[...]).astype(low)

    def grad_tiles(made, send_to, base, make):
        for n in range(dim // vw):
            tile = pl.ds(n * vw, vw)
            made[0:half, tile] = make(tile)
        return [
            remote(
                made.at[:, pl.ds(pl.multiple_of(side * width + oc * vw, vw), vw)],
                send_to.at[:, pl.ds(side * vw, vw)],
                dsend, drecv, base + side, partner,
            )
            for side in range(2)
        ]

    def make_two(tile):
        b = jnp.dot(gp_low[...], w_head[:, tile], preferred_element_type=wide)
        return (b * pre_two[:, tile]).astype(low)

    two_copies = grad_tiles(g_two, p_two, 5, make_two)

    def make_one(tile):
        b = lax.dot_general(
            g_two[0:half, :], w_two[tile, :], (((1,), (1,)), ((), ())), preferred_element_type=wide
        )
        return (b * pre_one[:, tile]).astype(low)

    one_copies = grad_tiles(g_one, p_one, 7, make_one)

    def both(made, came, a):
        own_cols = [
            made[:, pl.ds(pl.multiple_of(n * width + core * vw + a * TILE, TILE), TILE)] for n in range(2)
        ]
        par_cols = [came[:, n * vw + a * TILE : n * vw + (a + 1) * TILE] for n in range(2)]
        return jnp.concatenate(own_cols, axis=1), jnp.concatenate(par_cols, axis=1)

    def token_rows(side, first, size, out, base=0):
        for n in range(width // vw):
            b = lax.dot_general(
                g_one[first : first + size, :],
                w_one[pl.ds(pl.multiple_of(side * width + n * vw, vw), vw), :],
                (((1,), (1,)), ((), ())),
                preferred_element_type=wide,
            )
            place_rows = pl.ds(pl.multiple_of(base + first, 16), size)
            out[place_rows, n * vw : (n + 1) * vw] = b.astype(low)

    results = (hb, o_two, o_two, o_one, o_one)
    tails = []
    waited = set()
    for name in STEPS:
        kind, args = name[0], [int(c) for c in name[1:]]
        if kind == "C":
            token_rows(other, 0, half, tg_far)
        elif kind == "T":
            first = args[0] * step
            place_out = o_tok.at[pl.ds(pl.multiple_of(x * half + first, 16), step), :]
            tails.append(remote(tg_far.at[pl.ds(first, step), :], place_out, xsend, xrecv, 5 + args[0], across))
        elif kind == "N":
            token_rows(x, 0, half, o_tok, x * half)
        elif kind == "P":
            g, h = args
            which = g > 2
            if which not in waited:
                waited.add(which)
                for copy in (one_copies + [flips[2]]) if which else (two_copies + [flips[1]]):
                    copy.wait_recv()
            sources = both(g_one, p_one, g - 3) if which else both(g_two, p_two, g - 1)
            state[g, h] = produce(g, h, t_tok if which else t_one, *sources)
        elif kind == "A":
            g, h, n = args
            state[g, h] = advance(g, h, n, state[g, h])
        elif kind == "L":
            (g,) = args
            state[g] = advance_last(g, [state[g, 0], state[g, 1]])
        else:
            (g,) = args
            finish(g, state[g], results[g], TILE if g in (2, 4) else 0)
            if g == 0:
                coef_here = jnp.where(x == 0, coef[:, :vw], coef[:, vw:])
                o_head[...] = (hb[...] * coef_here)[:, 0:rows]
    for copy in tails:
        copy.wait_recv()
    for copy in started:
        copy.wait_send()


def fused(scale, kinds, land, tokens, first, second, head, targets):
    count, width = tokens.shape
    dim = first.shape[0]
    rows = head.shape[0]
    half = count // 2
    pad = -(-half // TILE) * TILE
    vw = 2 * TILE
    hr = TILE // 2
    low, wide = jnp.bfloat16, jnp.float32
    shape = jax.ShapeDtypeStruct
    slices = SLICES
    vm = pltpu.VMEM
    scratch = [
        vm((dim, dim), low), vm((dim, dim), low), vm((2 * vw, dim), low), vm((pad, dim), low),
        vm((half, width), low), vm((rows, count), wide), vm((rows, pad), low), vm((2, vw, pad), low),
        vm((TILE, count), wide), vm((half, 2 * vw), wide),
        vm((half, dim), wide), vm((half, dim), wide), vm((pad, dim), low), vm((pad, dim), low),
        vm((2, dim, pad), low), vm((2, dim, pad), low), vm((2, dim, pad), low),
        vm((pad, 2 * vw), wide), vm((half, 2 * vw), wide), vm((pad, 2 * vw), low), vm((pad, vw), low),
        vm((half, 2 * vw), low),
        vm((pad, dim), low), vm((pad, dim), low), vm((pad, width), low), vm((pad, width), low),
        vm((half, width), low), vm((hr, vw), wide),
        vm((8, TILE), wide), vm((8, TILE), wide),
        vm((8, TILE), wide), vm((8, 8, TILE), wide), vm((4, 8, TILE), wide), vm((8, TILE), wide),
        vm((slices, 2, hr, TILE), low), vm((slices, hr, TILE), wide),
        vm((slices, hr, TILE), low), vm((slices, hr, TILE), low),
    ]
    for kind in (low, low, wide):
        for key in sorted(PLAN):
            scratch += [vm(found, kind) for found in stage_shapes(PLAN[key])[:2]]
    scratch += [vm((slices, 2, 2, hr, TILE), kind) for kind in (low, low, wide)]
    sizes = (6, 48, 48, 7, 7, 9, 9, 10, 10, 9 * slices, 9 * slices)
    scratch += [pltpu.SemaphoreType.DMA((n,)) for n in sizes]
    return pl.pallas_call(
        fused_kernel,
        out_shape=(
            vm((8, TILE), wide),
            vm((count, width), low),
            vm((dim // 16, width), wide),
            vm((dim // 16, width), wide),
            vm((hr, rows), wide),
        ),
        in_specs=[pl.BlockSpec(memory_space=pltpu.SMEM), VMEM, VMEM] + [HBM] * 5,
        out_specs=[VMEM] * 5,
        scratch_shapes=scratch,
        compiler_params=params(0, 56),
        name="fused",
    )(scale, kinds, land, tokens, first, second, head, targets)


CHUNKS = 4


def write_kernel(loss, tok, one, two, head, o_loss, o_tok, o_one, o_two, o_head, f_loss, f_tok, went):
    size = tok.shape[0] // CHUNKS
    stores = []

    def store(src, dst):
        copy = pltpu.make_async_copy(src, dst, went.at[len(stores)])
        copy.start()
        stores.append(copy)

    store(one, o_one)
    store(two, o_two)
    store(head, o_head)
    f_loss[...] = loss[0:1, 0:1]
    store(f_loss, o_loss)
    for n in range(CHUNKS):
        span = pl.ds(n * size, size)
        f_tok[span, :] = tok[span, :].astype(jnp.float32)
        store(f_tok.at[span, :], o_tok.at[span, :])
    for copy in stores:
        copy.wait()


def write(*parts):
    wide = jnp.float32
    shapes = [(1, 1)] + [p.shape for p in parts[1:]]
    vm = pltpu.VMEM
    return pl.pallas_call(
        write_kernel,
        out_shape=tuple(jax.ShapeDtypeStruct(a, wide) for a in shapes),
        in_specs=[VMEM] * 5,
        out_specs=[ANY] * 5,
        scratch_shapes=[vm((1, 1), wide), vm(parts[1].shape, wide), pltpu.SemaphoreType.DMA((CHUNKS + 4,))],
        compiler_params=pltpu.CompilerParams(vmem_limit_bytes=16 * 2**20),
        name="write",
    )(*parts)


def per_device(
    tokens, first_weight, second_weight, head_weight, targets, land_mask, variable_kind, loss_scale
):
    parts = fused(
        loss_scale.reshape(1), variable_kind.reshape(1, -1), land_mask,
        tokens, first_weight, second_weight, head_weight, targets,
    )
    loss, token_grad, first_grad, second_grad, head_grad = write(*parts)
    return (loss.reshape(()), token_grad, first_grad, second_grad, head_grad.T)


def column_folder(weights, piece):
    return lax.dot_general(
        piece, weights, (((1,), (1,)), ((), ())), preferred_element_type=jnp.float32
    )


def row_folder(weights, piece):
    return lax.dot_general(
        piece, weights, (((0,), (0,)), ((), ())), preferred_element_type=jnp.float32
    )


def per_device_wide(
    tokens, first_weight, second_weight, head_weight, targets, land_mask, variable_kind, loss_scale
):
    count = tokens.shape[0]
    width = first_weight.shape[1]
    kinds = head_weight.shape[0] // PP
    rows_first, rows_second = (
        lax.all_to_all(first_weight, "tensor", split_axis=0, concat_axis=1, tiled=True),
        lax.all_to_all(second_weight, "tensor", split_axis=0, concat_axis=1, tiled=True),
    )
    head_cols = lax.all_to_all(head_weight, "tensor", split_axis=1, concat_axis=0, tiled=True)
    position = lax.axis_index("space") * count + jnp.arange(count, dtype=jnp.int32)
    cell = jnp.arange(PP, dtype=jnp.int32)
    lat_row = 2 * (position // LONP)[None, :] + (cell // 2)[:, None]
    nlat = 2 * PROW_DEV * lax.axis_size("space")
    cell_weight = jnp.cos(math.pi / 2.0 * (lat_row.astype(jnp.float32) + 0.5) / nlat)
    land = land_mask.astype(jnp.float32)
    kind = variable_kind[:, None, None]
    valid = jnp.where(kind == 0, 1.0, jnp.where(kind == 1, land[None], 1.0 - land[None]))
    masked = cell_weight[None] * valid
    local_weight = jnp.sum(masked, axis=(1, 2))
    weight_sum = lax.psum(local_weight, "space")
    full_in = lax.all_gather(tokens, "tensor", axis=1, tiled=True)
    pre_one = jnp.dot(full_in, first_weight, preferred_element_type=jnp.float32)
    hidden_one = jax.nn.gelu(pre_one, approximate=False).astype(jnp.bfloat16)
    full_one = lax.all_gather(hidden_one, "tensor", axis=1, tiled=True)
    pre_two = jnp.dot(full_one, second_weight, preferred_element_type=jnp.float32)
    hidden_two = jax.nn.gelu(pre_two, approximate=False).astype(jnp.bfloat16)
    full_two = lax.all_gather(hidden_two, "tensor", axis=1, tiled=True)
    predicted = lax.dot_general(
        head_weight, full_two, (((1,), (1,)), ((), ())), preferred_element_type=jnp.float32
    )
    error = predicted.reshape(kinds, PP, count) - targets.reshape(kinds, PP, count)
    local_error = jnp.sum(masked * error * error, axis=(1, 2))
    error_sum = lax.psum(local_error, "space")
    root = jnp.sqrt(error_sum / weight_sum + 1e-06)
    loss = lax.psum(jnp.sum(root), "tensor") / (kinds * lax.axis_size("tensor"))
    coef = loss_scale / (kinds * lax.axis_size("tensor") * root * weight_sum)
    grad_pred = (
        (coef[:, None, None] * masked * error).reshape(kinds * PP, count).astype(jnp.bfloat16)
    )
    back_two = row_folder(head_cols, lax.all_gather(grad_pred, "tensor", axis=0, tiled=True))
    head_term = jnp.dot(grad_pred, full_two, preferred_element_type=jnp.float32)
    head_grad = lax.psum_scatter(head_term, "space", scatter_dimension=1, tiled=True)
    grad_two = (back_two * slope(pre_two)).astype(jnp.bfloat16)
    back_one = column_folder(rows_second, lax.all_gather(grad_two, "tensor", axis=1, tiled=True))
    grad_one = (back_one * slope(pre_one)).astype(jnp.bfloat16)
    joined = lax.psum_scatter(
        jnp.concatenate(
            [
                lax.dot_general(
                    full_one, grad_two, (((0,), (0,)), ((), ())), preferred_element_type=jnp.float32
                ),
                lax.dot_general(
                    full_in, grad_one, (((0,), (0,)), ((), ())), preferred_element_type=jnp.float32
                ),
            ],
            axis=1,
        ),
        "space",
        scatter_dimension=0,
        tiled=True,
    )
    second_grad = joined[:, :width]
    first_grad = joined[:, width:]
    token_grad = column_folder(rows_first, lax.all_gather(grad_one, "tensor", axis=1, tiled=True))
    return (loss, token_grad, first_grad, second_grad, head_grad)


def solution(mesh):
    size = mesh.shape["space"]
    paired = mesh.shape["tensor"] == 2 and size == 16
    return jax.shard_map(
        per_device if paired else per_device_wide,
        mesh=mesh,
        in_specs=(
            P("space", "tensor"),
            P(None, "tensor"),
            P(None, "tensor"),
            P("tensor", None),
            P("tensor", "space"),
            P(None, "space"),
            P("tensor"),
            P(),
        ),
        out_specs=(
            P(),
            P("space", "tensor"),
            P("space", "tensor"),
            P("space", "tensor"),
            P("tensor", "space"),
        ),
        check_vma=False,
    )
```

```python
import math

import jax
import jax.numpy as jnp
from jax import lax
from jax.experimental import pallas as pl
from jax.experimental.pallas import tpu as pltpu
from jax.sharding import PartitionSpec as P

PP = 4
PROW_DEV = 4
LONP = 224
MESH = pl.DeviceIdType.MESH
VMEM = pl.BlockSpec(memory_space=pltpu.VMEM)
ANY = pl.BlockSpec(memory_space=pl.ANY)


def bent(z):
    return (0.5 * z * (1.0 + lax.erf(z / math.sqrt(2.0)))).astype(jnp.bfloat16)


def slope(z):
    cdf = 0.5 * (1.0 + lax.erf(z / math.sqrt(2.0)))
    return cdf + z * jnp.exp(-0.5 * z * z) / math.sqrt(2.0 * math.pi)


def flipped(s, bit):
    step = 1 << bit
    return s + step - 2 * step * ((s // step) % 2)


def greet(partners):
    barrier = pltpu.get_barrier_semaphore()
    for partner in partners:
        pl.semaphore_signal(barrier, inc=1, device_id=partner, device_id_type=MESH)
    pl.semaphore_wait(barrier, len(partners))


def params(number, mib):
    return pltpu.CompilerParams(
        collective_id=number, has_side_effects=True, vmem_limit_bytes=mib * 2**20
    )


HBM = pl.BlockSpec(memory_space=pltpu.HBM)
TILE = 128
TREES = ((2, 1, 0), (3, 2, 1, 0), (1, 3, 2, 0), (1, 2, 0))
SLICES = 5
BITS = {"z": 2, "y": 1}
PLAN = {
    (0, 0): "yzx", (0, 1): "yxz", (1, 0): "yzx", (1, 1): "zyx", (2, 0): "zyx", (2, 1): "yxz", (3, 0): "yzx",
    (3, 1): "zxy", (4, 0): "zyx", (4, 1): "yxz",
}
STEPS = (
    "C", "A001", "T0", "P21", "P11", "T1", "P10", "A011", "P20", "P30", "A002", "P41", "P31", "P40", "A211",
    "A111", "A101", "A201", "N", "A301", "A311", "A012", "A411", "A401", "A212", "A112", "A102", "A312",
    "A202", "A302", "A412", "L0", "A402", "L1", "L2", "L3", "L4", "F0", "F1", "F2", "F3", "F4",
)


def stage_shapes(order):
    found = []
    left, lanes = 3, 2 * TILE
    for way in order:
        if way == "x":
            lanes = TILE
        else:
            left -= 1
        found.append((2,) * left + (TILE // 2, lanes))
    return found


def fused_kernel(
    scale, kinds_in, land, tok, one, two, head, tar,
    o_loss, o_tok, o_one, o_two, o_head,
    w_one, w_two, w_head, toks, tok_out, tar_v, tar_s, tar_all, lnd, masked,
    pre_one, pre_two, h_one, h_two, t_tok, t_one, t_two, tgt, scored, sc_low, sc_par, gp_low,
    g_two, g_one, p_two, p_one, tg_far, hb, kb, kp,
    msg, near, far, mid, finals, arrs3, arrs4, arrs5, *refs,
):
    keys = sorted(PLAN)
    pick_refs = iter(refs)
    fars, arrs, nears = [{key: [next(pick_refs), next(pick_refs)] for key in keys} for _ in range(3)]
    fars2, arrs2, nears2 = [next(pick_refs) for _ in range(3)]
    for store, final in ((fars, fars2), (arrs, arrs2), (nears, nears2)):
        for g, h in keys:
            store[g, h].append(final.at[g, h])
    local, wsend, wrecv, xsend, xrecv, dsend, drecv, tsend, trecv, rsend, rrecv = pick_refs
    low, wide = jnp.bfloat16, jnp.float32
    s, x = lax.axis_index("space"), lax.axis_index("tensor")
    other = 1 - x
    zf, zn, yy, core = (s // 8) % 2, (s // 4) % 2, (s // 2) % 2, s % 2
    oc = 1 - core
    count = tok.shape[0]
    half = count // 2
    dim, width = one.shape
    rows = head.shape[0]
    pad = toks.shape[0]
    vw = 2 * TILE
    hr = TILE // 2
    across, partner = (s, other), (flipped(s, 0), x)
    diagonal = (flipped(flipped(s, 3), 0), x)
    started = []

    def at(index, size):
        return pl.ds(pl.multiple_of(index * size, size), size)

    def remote(src, dst, sends, recvs, slot, target):
        copy = pltpu.make_async_remote_copy(
            src_ref=src,
            dst_ref=dst,
            send_sem=sends.at[slot],
            recv_sem=recvs.at[slot],
            device_id=target,
            device_id_type=MESH,
        )
        copy.start()
        started.append(copy)
        return copy

    moves = [
        (one, w_one.at[:, at(x, width)]),
        (two, w_two.at[:, at(x, width)]),
        (head, w_head.at[pl.ds(pl.multiple_of(x * vw, vw), rows), :]),
        (tok.at[at(other, half), :], tok_out),
        (tar, tar_v),
        (tok.at[at(x, half), :], toks.at[pl.ds(0, half), at(x, width)]),
    ]
    loads = [pltpu.make_async_copy(a, b, local.at[n]) for n, (a, b) in enumerate(moves)]
    for copy in loads:
        copy.start()

    shard = 96
    w_head[pl.ds(pl.multiple_of(x * vw + rows, 16), vw - rows), :] = jnp.zeros((vw - rows, dim), low)
    w_head[pl.ds(pl.multiple_of(other * vw + 2 * shard, 16), vw - 2 * shard), :] = jnp.zeros(
        (vw - 2 * shard, dim), low
    )
    for ref in (toks, h_one, h_two, g_two, g_one, sc_low):
        ref[half:, :] = jnp.zeros((pad - half, ref.shape[1]), low)
    tar_all[:, rows:, :] = jnp.zeros((2, vw - rows, pad), low)
    kb[...] = jnp.zeros_like(kb)
    kb[0:1, 0 : rows // PP] = kinds_in[...].astype(wide)
    lnd[...] = jnp.zeros_like(lnd)
    lnd[0:PP, :] = land[...].astype(wide)

    low_bits, high = s % 4, s // 4
    mine = x * 4 + low_bits

    def near_peer(d):
        j = (mine + d) % 8
        return (high * 4 + j % 4, j // 4)

    def far_peer(d):
        return (((high + d) % 4) * 4 + low_bits, x)

    greet([near_peer(d) for d in range(1, 8)] + [far_peer(d) for d in range(1, 4)] + [diagonal])

    part = dim // 16

    def place(k, m, side):
        q = s
        for b in range(4):
            if (m >> b) & 1:
                q = flipped(q, b)
        if k in (0, 3):
            first = pl.multiple_of((q % 8) * 2 * part + (part if k == 3 else 0), part)
            return w_one.at[pl.ds(first, part), at(side, width)]
        if k == 1:
            return w_two.at[at(q, part), at(side, width)]
        first = pl.multiple_of(side * vw + (q % 2) * shard, 16)
        return w_head.at[pl.ds(first, shard), at(q // 2, TILE)]

    pieces = {}
    for k in (0, 3, 1, 2):
        if k < 3:
            loads[k].wait()
        pieces[k, 0] = remote(place(k, 0, x), place(k, 0, x), wsend, wrecv, 16 * k, across)
    kind_copy = remote(kb, kp, xsend, xrecv, 4, across)
    loads[3].wait()
    parts = 2
    step = half // parts
    tok_copies = [
        remote(
            tok_out.at[pl.ds(n * step, step), :],
            toks.at[pl.ds(n * step, step), at(x, width)],
            xsend, xrecv, n, across,
        )
        for n in range(parts)
    ]
    loads[4].wait()
    tail = count - pad
    lo = tar_v[:, :pad]
    hi = pltpu.roll(tar_v[:, tail:], pad - half + tail, 1)
    tar_s[...] = jnp.where(x == 0, hi, lo).astype(low)
    tar_copy = remote(tar_s, tar_all.at[x, pl.ds(0, rows), :], xsend, xrecv, parts, across)
    tar_all[x, 0:rows, :] = jnp.where(x == 0, lo, hi).astype(low)
    loads[5].wait()

    def relay(k, *ms):
        for m in ms:
            pieces[k, m].wait_recv()
            last = -1
            for n, b in enumerate(TREES[k]):
                if (m >> b) & 1:
                    last = n
            for b in TREES[k][last + 1 :]:
                piece = place(k, m, other)
                new = m ^ (1 << b)
                pieces[k, new] = remote(piece, piece, wsend, wrecv, 16 * k + new, (flipped(s, b), x))

    def layer(src, first, size, weight, side, pre, dst):
        span = slice(first, first + size)
        for i in range(width // vw):
            tile = pl.ds(pl.multiple_of(side * width + i * vw, vw), vw)
            z = jnp.dot(src[span, :], weight[:, tile], preferred_element_type=wide)
            pre[span, tile] = z
            dst[span, tile] = bent(z)

    def flip_to(src, dst, slot):
        for n in range(dim // TILE):
            dst[0, n * TILE : (n + 1) * TILE, :] = src[:, n * TILE : (n + 1) * TILE].T
        return remote(dst.at[0], dst.at[1], dsend, drecv, slot, partner)

    def make_slope(ref):
        def body(n, _):
            ref[:, at(n, TILE)] = slope(ref[:, at(n, TILE)])
            return 0

        lax.fori_loop(0, dim // TILE, body, 0)

    relay(0, 0)
    relay(3, 0)
    relay(1, 0)
    relay(2, 0)
    kind_copy.wait_recv()
    lane = lax.broadcasted_iota(jnp.int32, (1, 2 * vw), 1)
    used = lane % vw < rows
    cell = lane % PP
    group_shape = (TILE, vw)
    group = lax.broadcasted_iota(jnp.int32, group_shape, 1) // PP == lax.broadcasted_iota(jnp.int32, group_shape, 0)
    group = jnp.where(group, 1.0, 0.0).astype(low)
    k_own = jnp.dot(kb[...].astype(low), group, preferred_element_type=wide)[0:1, :]
    k_oth = jnp.dot(kp[...].astype(low), group, preferred_element_type=wide)[0:1, :]
    kind = jnp.concatenate([jnp.where(x == 0, k_own, k_oth), jnp.where(x == 0, k_oth, k_own)], axis=1)
    ground = jnp.where(x == 0, lnd[:, :pad], pltpu.roll(lnd[:, tail:], pad - half + tail, 1))
    pick_shape = (TILE, 2 * vw)
    pick = lax.broadcasted_iota(jnp.int32, pick_shape, 1) % PP == lax.broadcasted_iota(jnp.int32, pick_shape, 0)
    spread = jnp.dot(
        ground.T.astype(low), jnp.where(pick, 1.0, 0.0).astype(low), preferred_element_type=wide
    )
    bands = half // LONP
    nlat = 2 * (count // LONP) * lax.axis_size("space")
    for j in range(bands):
        lat_row = 2 * (s * (count // LONP) + x * bands + j) + cell // 2
        weight = jnp.cos(math.pi / 2.0 * (lat_row.astype(wide) + 0.5) / nlat)
        weight = jnp.where(used, weight, 0.0)
        flat = jnp.where(kind == 1.0, 0.0, weight)
        slant = jnp.where(kind == 1.0, weight, jnp.where(kind == 2.0, -weight, 0.0))
        band = slice(j * LONP, (j + 1) * LONP)
        masked[band, :] = flat + slant * spread[band, :]
    relay(0, 4, 2)
    relay(3, 2, 4)
    relay(1, 2, 4)
    relay(2, 2)
    relay(1, 8)
    tgt[:, at(x, vw)] = tar_all[x].astype(wide).T
    relay(2, 4, 8)
    tok_copies[0].wait_recv()
    layer(toks, 0, step, w_one, x, pre_one, h_one)
    relay(0, 6)
    relay(3, 6)
    relay(1, 12)
    relay(2, 6)
    relay(0, 1, 5, 3, 7)
    relay(3, 1, 5, 3, 7)
    layer(toks, 0, step, w_one, other, pre_one, h_one)
    relay(1, 6)
    relay(2, 10, 12)
    tok_copies[1].wait_recv()
    layer(toks, step, half - step, w_one, x, pre_one, h_one)
    layer(toks, step, half - step, w_one, other, pre_one, h_one)
    relay(1, 10, 14)
    layer(h_one, 0, half, w_two, x, pre_two, h_two)
    relay(2, 14)
    relay(1, 1, 9, 5, 13, 3, 11, 7, 15)
    layer(h_one, 0, half, w_two, other, pre_two, h_two)
    relay(2, 1, 9, 5, 13, 3, 11, 7, 15)
    tar_copy.wait_recv()
    tgt[:, at(other, vw)] = tar_all[other].astype(wide).T
    for side in range(2):
        cols = slice(side * vw, (side + 1) * vw)
        error = lax.dot_general(
            h_two[0:half, :], w_head[cols, :], (((1,), (1,)), ((), ())), preferred_element_type=wide
        )
        error = error - tgt[0:half, cols]
        m = masked[:, cols]
        sc = m * error
        scored[:, cols] = sc
        sc_low[0:half, cols] = sc.astype(low)
        esum = jnp.sum(sc * error, axis=0, keepdims=True)
        wsum = jnp.sum(m, axis=0, keepdims=True)
        for n in range(2):
            r = side * 2 + n
            msg[r : r + 1, :] = esum[:, n * TILE : (n + 1) * TILE]
            msg[4 + r : 5 + r, :] = wsum[:, n * TILE : (n + 1) * TILE]

    def share(src, slots, me, peers, base):
        copies = [remote(src, slots.at[me], tsend, trecv, base + n, peer) for n, peer in enumerate(peers)]
        slots[me] = src[...]
        return copies

    first_share = share(msg, near, mine, [near_peer(d) for d in range(1, 8)], 0)

    def scored_cols(side, c):
        return pl.ds(pl.multiple_of(side * vw + c * TILE, TILE), TILE)

    score_copies = [
        remote(sc_low.at[:, scored_cols(n, oc)], sc_par.at[:, pl.ds(n * TILE, TILE)], dsend, drecv, n, partner)
        for n in range(2)
    ]
    flips = [flip_to(h_two, t_two, 2), flip_to(h_one, t_one, 3), flip_to(toks, t_tok, 4)]
    make_slope(pre_two)
    for copy in first_share:
        copy.wait_recv()
    mid[...] = jnp.sum(near[...], axis=0)
    second_share = share(mid, far, high, [far_peer(d) for d in range(1, 4)], 7)

    mark_bits = {"z": zn, "y": yy}

    def goal(way):
        return across if way == "x" else (flipped(s, BITS[way]), x)

    def produce(g, h, trans, own_cols, par_cols):
        first = PLAN[g, h][0]
        both_cols = jnp.concatenate([own_cols, par_cols], axis=0)
        ref, store = fars[g, h][0], nears[g, h][0]

        def product(blocks):
            sides = [
                jnp.concatenate(
                    [trans[k, pl.ds(pl.multiple_of(b * TILE + h * hr, hr), hr), :] for b in blocks], axis=0
                )
                for k in range(2)
            ]
            return jnp.dot(jnp.concatenate(sides, axis=1), both_cols, preferred_element_type=wide)

        def blocks_of(v):
            return [i * 4 + (j * 2 + v if first == "y" else v * 2 + j) for i in range(2) for j in range(2)]

        if first == "x":
            out = product(list(range(8)))
            ref[...] = jnp.where(x == 0, out[:, TILE:], out[:, :TILE]).astype(low).reshape(ref.shape)
            store[...] = jnp.where(x == 0, out[:, :TILE], out[:, TILE:]).reshape(ref.shape)
        else:
            value = mark_bits[first]
            out = product(blocks_of(1 - value) + blocks_of(value))
            ref[...] = out[: 4 * hr].astype(low).reshape(ref.shape)
        copy = remote(ref, arrs[g, h][0], rsend, rrecv, 9 * g + 3 * h, goal(first))
        if first != "x":
            store[...] = out[4 * hr :].reshape(ref.shape)
        return copy

    def advance(g, h, n, copy):
        copy.wait_recv()
        order = PLAN[g, h]
        way = order[n]
        left = [d for d in "fzy" if d not in order[:n]]
        ref, came = nears[g, h][n - 1], arrs[g, h][n - 1]
        if way == "x":
            lead = (slice(None),) * (len(left) + 1)
            away, here = lead + (at(other, TILE),), lead + (at(x, TILE),)
        else:
            lead = (slice(None),) * left.index(way)
            away, here = lead + (1 - mark_bits[way],), lead + (mark_bits[way],)
        fars[g, h][n][...] = (ref[away] + came[away].astype(wide)).astype(low)
        copy = remote(fars[g, h][n], arrs[g, h][n], rsend, rrecv, 9 * g + 3 * h + n, goal(way))
        nears[g, h][n][...] = ref[here] + came[here].astype(wide)
        return copy

    def advance_last(g, before):
        for h in range(2):
            before[h].wait_recv()
            finals[g, h] = (nears2[g, h, 1 - zf] + arrs2[g, h, 1 - zf].astype(wide)).astype(low)
        up = (flipped(s, 3), x)
        copies = [
            remote(finals.at[g, core], arrs4.at[g], rsend, rrecv, 9 * g + 6, up),
            remote(finals.at[g, oc], arrs5.at[g], rsend, rrecv, 9 * g + 7, diagonal),
        ]
        for h in range(2):
            nears2[g, h, zf] = nears2[g, h, zf] + arrs2[g, h, zf].astype(wide)
        copies.append(remote(nears2.at[g, oc, zf], arrs3.at[g], rsend, rrecv, 9 * g + 8, partner))
        return copies

    def finish(g, copies, out, base):
        for copy in copies:
            copy.wait_recv()
        kept = nears2[g, core, zf] + arrs4[g].astype(wide)
        came = arrs3[g] + arrs5[g].astype(wide)
        span = out.shape[1] // 2
        out[pl.ds(0, hr), pl.ds(pl.multiple_of(core * span + base, TILE), TILE)] = kept
        out[pl.ds(0, hr), pl.ds(pl.multiple_of(oc * span + base, TILE), TILE)] = came

    for copy in score_copies:
        copy.wait_recv()
    flips[0].wait_recv()
    state = {}
    own = jnp.concatenate([sc_low[:, scored_cols(n, core)] for n in range(2)], axis=1)
    for h in range(2):
        state[0, h] = produce(0, h, t_two, own, sc_par[...])
    make_slope(pre_one)
    for copy in second_share:
        copy.wait_recv()
    sums = jnp.sum(far[...], axis=0)
    tl = lax.broadcasted_iota(jnp.int32, (8, TILE), 1)
    sums = sums + jnp.where(tl % 2 == 0, pltpu.roll(sums, TILE - 1, 1), pltpu.roll(sums, 1, 1))
    sums = sums + jnp.where(tl % 4 < 2, pltpu.roll(sums, TILE - 2, 1), pltpu.roll(sums, 2, 1))
    kinds = 2 * rows // PP
    line = lax.broadcasted_iota(jnp.int32, (4, TILE), 0)
    tl = lax.broadcasted_iota(jnp.int32, (4, TILE), 1)
    ok = (line % 2) * TILE + tl < rows
    weight_sum = jnp.where(ok, sums[4:8, :], 1.0)
    root = jnp.sqrt(jnp.where(ok, sums[0:4, :], 0.0) / weight_sum + 1e-06)
    roots = jnp.where(ok & (tl % PP == 0), root, 0.0)
    loss = jnp.sum(jnp.sum(roots, axis=0, keepdims=True), axis=1, keepdims=True) / kinds
    o_loss[...] = jnp.broadcast_to(loss, o_loss.shape)
    coef = jnp.where(ok, scale[0] / (kinds * root * weight_sum), 0.0)
    coef = jnp.concatenate([coef[n : n + 1, :] for n in range(4)], axis=1)
    gp_low[...] = (coef * scored[...]).astype(low)

    def grad_tiles(made, send_to, base, make):
        for n in range(dim // vw):
            tile = pl.ds(n * vw, vw)
            made[0:half, tile] = make(tile)
        return [
            remote(
                made.at[:, pl.ds(pl.multiple_of(side * width + oc * vw, vw), vw)],
                send_to.at[:, pl.ds(side * vw, vw)],
                dsend, drecv, base + side, partner,
            )
            for side in range(2)
        ]

    def make_two(tile):
        b = jnp.dot(gp_low[...], w_head[:, tile], preferred_element_type=wide)
        return (b * pre_two[:, tile]).astype(low)

    two_copies = grad_tiles(g_two, p_two, 5, make_two)

    def make_one(tile):
        b = lax.dot_general(
            g_two[0:half, :], w_two[tile, :], (((1,), (1,)), ((), ())), preferred_element_type=wide
        )
        return (b * pre_one[:, tile]).astype(low)

    one_copies = grad_tiles(g_one, p_one, 7, make_one)

    def both(made, came, a):
        own_cols = [
            made[:, pl.ds(pl.multiple_of(n * width + core * vw + a * TILE, TILE), TILE)] for n in range(2)
        ]
        par_cols = [came[:, n * vw + a * TILE : n * vw + (a + 1) * TILE] for n in range(2)]
        return jnp.concatenate(own_cols, axis=1), jnp.concatenate(par_cols, axis=1)

    def token_rows(side, first, size, out, base=0):
        for n in range(width // vw):
            b = lax.dot_general(
                g_one[first : first + size, :],
                w_one[pl.ds(pl.multiple_of(side * width + n * vw, vw), vw), :],
                (((1,), (1,)), ((), ())),
                preferred_element_type=wide,
            )
            place_rows = pl.ds(pl.multiple_of(base + first, 16), size)
            out[place_rows, n * vw : (n + 1) * vw] = b.astype(low)

    results = (hb, o_two, o_two, o_one, o_one)
    tails = []
    waited = set()
    for name in STEPS:
        kind, args = name[0], [int(c) for c in name[1:]]
        if kind == "C":
            token_rows(other, 0, half, tg_far)
        elif kind == "T":
            first = args[0] * step
            place_out = o_tok.at[pl.ds(pl.multiple_of(x * half + first, 16), step), :]
            tails.append(remote(tg_far.at[pl.ds(first, step), :], place_out, xsend, xrecv, 5 + args[0], across))
        elif kind == "N":
            token_rows(x, 0, half, o_tok, x * half)
        elif kind == "P":
            g, h = args
            which = g > 2
            if which not in waited:
                waited.add(which)
                for copy in (one_copies + [flips[2]]) if which else (two_copies + [flips[1]]):
                    copy.wait_recv()
            sources = both(g_one, p_one, g - 3) if which else both(g_two, p_two, g - 1)
            state[g, h] = produce(g, h, t_tok if which else t_one, *sources)
        elif kind == "A":
            g, h, n = args
            state[g, h] = advance(g, h, n, state[g, h])
        elif kind == "L":
            (g,) = args
            state[g] = advance_last(g, [state[g, 0], state[g, 1]])
        else:
            (g,) = args
            finish(g, state[g], results[g], TILE if g in (2, 4) else 0)
            if g == 0:
                coef_here = jnp.where(x == 0, coef[:, :vw], coef[:, vw:])
                o_head[...] = (hb[...] * coef_here)[:, 0:rows]
    for copy in tails:
        copy.wait_recv()
    for copy in started:
        copy.wait_send()


def fused(scale, kinds, land, tokens, first, second, head, targets):
    count, width = tokens.shape
    dim = first.shape[0]
    rows = head.shape[0]
    half = count // 2
    pad = -(-half // TILE) * TILE
    vw = 2 * TILE
    hr = TILE // 2
    low, wide = jnp.bfloat16, jnp.float32
    shape = jax.ShapeDtypeStruct
    slices = SLICES
    vm = pltpu.VMEM
    scratch = [
        vm((dim, dim), low), vm((dim, dim), low), vm((2 * vw, dim), low), vm((pad, dim), low),
        vm((half, width), low), vm((rows, count), wide), vm((rows, pad), low), vm((2, vw, pad), low),
        vm((TILE, count), wide), vm((half, 2 * vw), wide),
        vm((half, dim), wide), vm((half, dim), wide), vm((pad, dim), low), vm((pad, dim), low),
        vm((2, dim, pad), low), vm((2, dim, pad), low), vm((2, dim, pad), low),
        vm((pad, 2 * vw), wide), vm((half, 2 * vw), wide), vm((pad, 2 * vw), low), vm((pad, vw), low),
        vm((half, 2 * vw), low),
        vm((pad, dim), low), vm((pad, dim), low), vm((pad, width), low), vm((pad, width), low),
        vm((half, width), low), vm((hr, vw), wide),
        vm((8, TILE), wide), vm((8, TILE), wide),
        vm((8, TILE), wide), vm((8, 8, TILE), wide), vm((4, 8, TILE), wide), vm((8, TILE), wide),
        vm((slices, 2, hr, TILE), low), vm((slices, hr, TILE), wide),
        vm((slices, hr, TILE), low), vm((slices, hr, TILE), low),
    ]
    for kind in (low, low, wide):
        for key in sorted(PLAN):
            scratch += [vm(found, kind) for found in stage_shapes(PLAN[key])[:2]]
    scratch += [vm((slices, 2, 2, hr, TILE), kind) for kind in (low, low, wide)]
    sizes = (6, 64, 64, 7, 7, 9, 9, 10, 10, 9 * slices, 9 * slices)
    scratch += [pltpu.SemaphoreType.DMA((n,)) for n in sizes]
    return pl.pallas_call(
        fused_kernel,
        out_shape=(
            vm((8, TILE), wide),
            vm((count, width), low),
            vm((dim // 16, width), wide),
            vm((dim // 16, width), wide),
            vm((hr, rows), wide),
        ),
        in_specs=[pl.BlockSpec(memory_space=pltpu.SMEM), VMEM, VMEM] + [HBM] * 5,
        out_specs=[VMEM] * 5,
        scratch_shapes=scratch,
        compiler_params=params(0, 56),
        name="fused",
    )(scale, kinds, land, tokens, first, second, head, targets)


CHUNKS = 4


def write_kernel(loss, tok, one, two, head, o_loss, o_tok, o_one, o_two, o_head, f_loss, f_tok, went):
    size = tok.shape[0] // CHUNKS
    stores = []

    def store(src, dst):
        copy = pltpu.make_async_copy(src, dst, went.at[len(stores)])
        copy.start()
        stores.append(copy)

    store(one, o_one)
    store(two, o_two)
    store(head, o_head)
    f_loss[...] = loss[0:1, 0:1]
    store(f_loss, o_loss)
    for n in range(CHUNKS):
        span = pl.ds(n * size, size)
        f_tok[span, :] = tok[span, :].astype(jnp.float32)
        store(f_tok.at[span, :], o_tok.at[span, :])
    for copy in stores:
        copy.wait()


def write(*parts):
    wide = jnp.float32
    shapes = [(1, 1)] + [p.shape for p in parts[1:]]
    vm = pltpu.VMEM
    return pl.pallas_call(
        write_kernel,
        out_shape=tuple(jax.ShapeDtypeStruct(a, wide) for a in shapes),
        in_specs=[VMEM] * 5,
        out_specs=[ANY] * 5,
        scratch_shapes=[vm((1, 1), wide), vm(parts[1].shape, wide), pltpu.SemaphoreType.DMA((CHUNKS + 4,))],
        compiler_params=pltpu.CompilerParams(vmem_limit_bytes=16 * 2**20),
        name="write",
    )(*parts)


def per_device(
    tokens, first_weight, second_weight, head_weight, targets, land_mask, variable_kind, loss_scale
):
    parts = fused(
        loss_scale.reshape(1), variable_kind.reshape(1, -1), land_mask,
        tokens, first_weight, second_weight, head_weight, targets,
    )
    loss, token_grad, first_grad, second_grad, head_grad = write(*parts)
    return (loss.reshape(()), token_grad, first_grad, second_grad, head_grad.T)


def column_folder(weights, piece):
    return lax.dot_general(
        piece, weights, (((1,), (1,)), ((), ())), preferred_element_type=jnp.float32
    )


def row_folder(weights, piece):
    return lax.dot_general(
        piece, weights, (((0,), (0,)), ((), ())), preferred_element_type=jnp.float32
    )


def per_device_wide(
    tokens, first_weight, second_weight, head_weight, targets, land_mask, variable_kind, loss_scale
):
    count = tokens.shape[0]
    width = first_weight.shape[1]
    kinds = head_weight.shape[0] // PP
    rows_first, rows_second = (
        lax.all_to_all(first_weight, "tensor", split_axis=0, concat_axis=1, tiled=True),
        lax.all_to_all(second_weight, "tensor", split_axis=0, concat_axis=1, tiled=True),
    )
    head_cols = lax.all_to_all(head_weight, "tensor", split_axis=1, concat_axis=0, tiled=True)
    position = lax.axis_index("space") * count + jnp.arange(count, dtype=jnp.int32)
    cell = jnp.arange(PP, dtype=jnp.int32)
    lat_row = 2 * (position // LONP)[None, :] + (cell // 2)[:, None]
    nlat = 2 * PROW_DEV * lax.axis_size("space")
    cell_weight = jnp.cos(math.pi / 2.0 * (lat_row.astype(jnp.float32) + 0.5) / nlat)
    land = land_mask.astype(jnp.float32)
    kind = variable_kind[:, None, None]
    valid = jnp.where(kind == 0, 1.0, jnp.where(kind == 1, land[None], 1.0 - land[None]))
    masked = cell_weight[None] * valid
    local_weight = jnp.sum(masked, axis=(1, 2))
    weight_sum = lax.psum(local_weight, "space")
    full_in = lax.all_gather(tokens, "tensor", axis=1, tiled=True)
    pre_one = jnp.dot(full_in, first_weight, preferred_element_type=jnp.float32)
    hidden_one = jax.nn.gelu(pre_one, approximate=False).astype(jnp.bfloat16)
    full_one = lax.all_gather(hidden_one, "tensor", axis=1, tiled=True)
    pre_two = jnp.dot(full_one, second_weight, preferred_element_type=jnp.float32)
    hidden_two = jax.nn.gelu(pre_two, approximate=False).astype(jnp.bfloat16)
    full_two = lax.all_gather(hidden_two, "tensor", axis=1, tiled=True)
    predicted = lax.dot_general(
        head_weight, full_two, (((1,), (1,)), ((), ())), preferred_element_type=jnp.float32
    )
    error = predicted.reshape(kinds, PP, count) - targets.reshape(kinds, PP, count)
    local_error = jnp.sum(masked * error * error, axis=(1, 2))
    error_sum = lax.psum(local_error, "space")
    root = jnp.sqrt(error_sum / weight_sum + 1e-06)
    loss = lax.psum(jnp.sum(root), "tensor") / (kinds * lax.axis_size("tensor"))
    coef = loss_scale / (kinds * lax.axis_size("tensor") * root * weight_sum)
    grad_pred = (
        (coef[:, None, None] * masked * error).reshape(kinds * PP, count).astype(jnp.bfloat16)
    )
    back_two = row_folder(head_cols, lax.all_gather(grad_pred, "tensor", axis=0, tiled=True))
    head_term = jnp.dot(grad_pred, full_two, preferred_element_type=jnp.float32)
    head_grad = lax.psum_scatter(head_term, "space", scatter_dimension=1, tiled=True)
    grad_two = (back_two * slope(pre_two)).astype(jnp.bfloat16)
    back_one = column_folder(rows_second, lax.all_gather(grad_two, "tensor", axis=1, tiled=True))
    grad_one = (back_one * slope(pre_one)).astype(jnp.bfloat16)
    joined = lax.psum_scatter(
        jnp.concatenate(
            [
                lax.dot_general(
                    full_one, grad_two, (((0,), (0,)), ((), ())), preferred_element_type=jnp.float32
                ),
                lax.dot_general(
                    full_in, grad_one, (((0,), (0,)), ((), ())), preferred_element_type=jnp.float32
                ),
            ],
            axis=1,
        ),
        "space",
        scatter_dimension=0,
        tiled=True,
    )
    second_grad = joined[:, :width]
    first_grad = joined[:, width:]
    token_grad = column_folder(rows_first, lax.all_gather(grad_one, "tensor", axis=1, tiled=True))
    return (loss, token_grad, first_grad, second_grad, head_grad)


def solution(mesh):
    size = mesh.shape["space"]
    paired = mesh.shape["tensor"] == 2 and size == 16
    return jax.shard_map(
        per_device if paired else per_device_wide,
        mesh=mesh,
        in_specs=(
            P("space", "tensor"),
            P(None, "tensor"),
            P(None, "tensor"),
            P("tensor", None),
            P("tensor", "space"),
            P(None, "space"),
            P("tensor"),
            P(),
        ),
        out_specs=(
            P(),
            P("space", "tensor"),
            P("space", "tensor"),
            P("space", "tensor"),
            P("tensor", "space"),
        ),
        check_vma=False,
    )
```

```python
import math

import jax
import jax.numpy as jnp
from jax import lax
from jax.experimental import pallas as pl
from jax.experimental.pallas import tpu as pltpu
from jax.sharding import PartitionSpec as P

PP = 4
PROW_DEV = 4
LONP = 224
MESH = pl.DeviceIdType.MESH
VMEM = pl.BlockSpec(memory_space=pltpu.VMEM)
ANY = pl.BlockSpec(memory_space=pl.ANY)


def bent(z):
    return (0.5 * z * (1.0 + lax.erf(z / math.sqrt(2.0)))).astype(jnp.bfloat16)


def slope(z):
    cdf = 0.5 * (1.0 + lax.erf(z / math.sqrt(2.0)))
    return cdf + z * jnp.exp(-0.5 * z * z) / math.sqrt(2.0 * math.pi)


def flipped(s, bit):
    step = 1 << bit
    return s + step - 2 * step * ((s // step) % 2)


def greet(partners):
    barrier = pltpu.get_barrier_semaphore()
    for partner in partners:
        pl.semaphore_signal(barrier, inc=1, device_id=partner, device_id_type=MESH)
    pl.semaphore_wait(barrier, len(partners))


def params(number, mib):
    return pltpu.CompilerParams(
        collective_id=number, has_side_effects=True, vmem_limit_bytes=mib * 2**20
    )


HBM = pl.BlockSpec(memory_space=pltpu.HBM)
TILE = 128
TREES = ((2, 1, 0), (3, 2, 1, 0), (1, 3, 2, 0), (1, 2, 0))
SLICES = 5
BITS = {"z": 2, "y": 1}
PLAN = {
    (0, 0): "xyz", (0, 1): "xzy", (1, 0): "yzx", (1, 1): "zxy", (2, 0): "yxz", (2, 1): "xzy", (3, 0): "yxz",
    (3, 1): "xyz", (4, 0): "zxy", (4, 1): "zyx",
}
STEPS = (
    "C", "P11", "T0", "A001", "P10", "P41", "P40", "A011", "P21", "P20", "P30", "A002", "P31", "A111",
    "A101", "A411", "A211", "N", "A201", "A401", "A311", "A012", "A301", "A112", "A412", "A202", "T1",
    "A102", "T2", "T3", "A312", "A402", "A212", "L0", "A302", "L4", "L2", "L3", "L1", "F0", "F4", "F2", "F3",
    "F1",
)


def stage_shapes(order):
    found = []
    left, lanes = 3, 2 * TILE
    for way in order:
        if way == "x":
            lanes = TILE
        else:
            left -= 1
        found.append((2,) * left + (TILE // 2, lanes))
    return found


def fused_kernel(
    scale, kinds_in, land, tok, one, two, head, tar,
    o_loss, o_tok, o_one, o_two, o_head,
    w_one, w_two, w_head, toks, tok_out, tar_v, tar_s, tar_all, lnd, masked,
    pre_one, pre_two, h_one, h_two, t_tok, t_one, t_two, tgt, scored, sc_low, sc_par, gp_low,
    g_two, g_one, p_two, p_one, tg_far, hb, kb, kp,
    msg, near, far, mid, finals, arrs3, arrs4, arrs5, *refs,
):
    keys = sorted(PLAN)
    pick_refs = iter(refs)
    fars, arrs, nears = [{key: [next(pick_refs), next(pick_refs)] for key in keys} for _ in range(3)]
    fars2, arrs2, nears2 = [next(pick_refs) for _ in range(3)]
    for store, final in ((fars, fars2), (arrs, arrs2), (nears, nears2)):
        for g, h in keys:
            store[g, h].append(final.at[g, h])
    local, wsend, wrecv, xsend, xrecv, dsend, drecv, tsend, trecv, rsend, rrecv = pick_refs
    low, wide = jnp.bfloat16, jnp.float32
    s, x = lax.axis_index("space"), lax.axis_index("tensor")
    other = 1 - x
    zf, zn, yy, core = (s // 8) % 2, (s // 4) % 2, (s // 2) % 2, s % 2
    oc = 1 - core
    count = tok.shape[0]
    half = count // 2
    dim, width = one.shape
    rows = head.shape[0]
    pad = toks.shape[0]
    vw = 2 * TILE
    hr = TILE // 2
    across, partner = (s, other), (flipped(s, 0), x)
    diagonal = (flipped(flipped(s, 3), 0), x)
    started = []

    def at(index, size):
        return pl.ds(pl.multiple_of(index * size, size), size)

    def remote(src, dst, sends, recvs, slot, target):
        copy = pltpu.make_async_remote_copy(
            src_ref=src,
            dst_ref=dst,
            send_sem=sends.at[slot],
            recv_sem=recvs.at[slot],
            device_id=target,
            device_id_type=MESH,
        )
        copy.start()
        started.append(copy)
        return copy

    moves = [
        (one, w_one.at[:, at(x, width)]),
        (two, w_two.at[:, at(x, width)]),
        (head, w_head.at[pl.ds(pl.multiple_of(x * vw, vw), rows), :]),
        (tok.at[at(other, half), :], tok_out),
        (tar, tar_v),
        (tok.at[at(x, half), :], toks.at[pl.ds(0, half), at(x, width)]),
    ]
    loads = [pltpu.make_async_copy(a, b, local.at[n]) for n, (a, b) in enumerate(moves)]
    for copy in loads:
        copy.start()

    shard = 96
    w_head[pl.ds(pl.multiple_of(x * vw + rows, 16), vw - rows), :] = jnp.zeros((vw - rows, dim), low)
    w_head[pl.ds(pl.multiple_of(other * vw + 2 * shard, 16), vw - 2 * shard), :] = jnp.zeros(
        (vw - 2 * shard, dim), low
    )
    for ref in (toks, h_one, h_two, g_two, g_one, sc_low):
        ref[half:, :] = jnp.zeros((pad - half, ref.shape[1]), low)
    tar_all[:, rows:, :] = jnp.zeros((2, vw - rows, pad), low)
    kb[...] = jnp.zeros_like(kb)
    kb[0:1, 0 : rows // PP] = kinds_in[...].astype(wide)
    lnd[...] = jnp.zeros_like(lnd)
    lnd[0:PP, :] = land[...].astype(wide)

    low_bits, high = s % 4, s // 4
    mine = x * 4 + low_bits

    def near_peer(d):
        j = (mine + d) % 8
        return (high * 4 + j % 4, j // 4)

    def far_peer(d):
        return (((high + d) % 4) * 4 + low_bits, x)

    greet([near_peer(d) for d in range(1, 8)] + [far_peer(d) for d in range(1, 4)] + [diagonal])

    part = dim // 16

    def place(k, m, side):
        q = s
        for b in range(4):
            if (m >> b) & 1:
                q = flipped(q, b)
        if k in (0, 3):
            first = pl.multiple_of((q % 8) * 2 * part + (part if k == 3 else 0), part)
            return w_one.at[pl.ds(first, part), at(side, width)]
        if k == 1:
            return w_two.at[at(q, part), at(side, width)]
        first = pl.multiple_of(side * vw + (q % 2) * shard, 16)
        return w_head.at[pl.ds(first, shard), at(q // 2, TILE)]

    pieces = {}
    for k in (0, 3, 1, 2):
        if k < 3:
            loads[k].wait()
        pieces[k, 0] = remote(place(k, 0, x), place(k, 0, x), wsend, wrecv, 16 * k, across)
    kind_copy = remote(kb, kp, xsend, xrecv, 4, across)
    loads[3].wait()
    parts = 2
    step = half // parts
    tok_copies = [
        remote(
            tok_out.at[pl.ds(n * step, step), :],
            toks.at[pl.ds(n * step, step), at(x, width)],
            xsend, xrecv, n, across,
        )
        for n in range(parts)
    ]
    loads[4].wait()
    tail = count - pad
    lo = tar_v[:, :pad]
    hi = pltpu.roll(tar_v[:, tail:], pad - half + tail, 1)
    tar_s[...] = jnp.where(x == 0, hi, lo).astype(low)
    tar_copy = remote(tar_s, tar_all.at[x, pl.ds(0, rows), :], xsend, xrecv, parts, across)
    tar_all[x, 0:rows, :] = jnp.where(x == 0, lo, hi).astype(low)
    loads[5].wait()

    def relay(k, *ms):
        for m in ms:
            pieces[k, m].wait_recv()
            last = -1
            for n, b in enumerate(TREES[k]):
                if (m >> b) & 1:
                    last = n
            for b in TREES[k][last + 1 :]:
                piece = place(k, m, other)
                new = m ^ (1 << b)
                pieces[k, new] = remote(piece, piece, wsend, wrecv, 16 * k + new, (flipped(s, b), x))

    def layer(src, first, size, weight, side, pre, dst):
        span = slice(first, first + size)
        for i in range(width // vw):
            tile = pl.ds(pl.multiple_of(side * width + i * vw, vw), vw)
            z = jnp.dot(src[span, :], weight[:, tile], preferred_element_type=wide)
            pre[span, tile] = z
            dst[span, tile] = bent(z)

    def flip_to(src, dst, slot):
        for n in range(dim // TILE):
            dst[0, n * TILE : (n + 1) * TILE, :] = src[:, n * TILE : (n + 1) * TILE].T
        return remote(dst.at[0], dst.at[1], dsend, drecv, slot, partner)

    def make_slope(ref):
        def body(n, _):
            ref[:, at(n, TILE)] = slope(ref[:, at(n, TILE)])
            return 0

        lax.fori_loop(0, dim // TILE, body, 0)

    relay(0, 0)
    relay(3, 0)
    relay(1, 0)
    relay(2, 0)
    kind_copy.wait_recv()
    lane = lax.broadcasted_iota(jnp.int32, (1, 2 * vw), 1)
    used = lane % vw < rows
    cell = lane % PP
    group_shape = (TILE, vw)
    group = lax.broadcasted_iota(jnp.int32, group_shape, 1) // PP == lax.broadcasted_iota(jnp.int32, group_shape, 0)
    group = jnp.where(group, 1.0, 0.0).astype(low)
    k_own = jnp.dot(kb[...].astype(low), group, preferred_element_type=wide)[0:1, :]
    k_oth = jnp.dot(kp[...].astype(low), group, preferred_element_type=wide)[0:1, :]
    kind = jnp.concatenate([jnp.where(x == 0, k_own, k_oth), jnp.where(x == 0, k_oth, k_own)], axis=1)
    ground = jnp.where(x == 0, lnd[:, :pad], pltpu.roll(lnd[:, tail:], pad - half + tail, 1))
    pick_shape = (TILE, 2 * vw)
    pick = lax.broadcasted_iota(jnp.int32, pick_shape, 1) % PP == lax.broadcasted_iota(jnp.int32, pick_shape, 0)
    spread = jnp.dot(
        ground.T.astype(low), jnp.where(pick, 1.0, 0.0).astype(low), preferred_element_type=wide
    )
    bands = half // LONP
    nlat = 2 * (count // LONP) * lax.axis_size("space")
    for j in range(bands):
        lat_row = 2 * (s * (count // LONP) + x * bands + j) + cell // 2
        weight = jnp.cos(math.pi / 2.0 * (lat_row.astype(wide) + 0.5) / nlat)
        weight = jnp.where(used, weight, 0.0)
        flat = jnp.where(kind == 1.0, 0.0, weight)
        slant = jnp.where(kind == 1.0, weight, jnp.where(kind == 2.0, -weight, 0.0))
        band = slice(j * LONP, (j + 1) * LONP)
        masked[band, :] = flat + slant * spread[band, :]
    relay(0, 4, 2)
    relay(3, 2, 4)
    relay(1, 2, 4)
    relay(2, 2)
    relay(1, 8)
    tgt[:, at(x, vw)] = tar_all[x].astype(wide).T
    relay(2, 4, 8)
    tok_copies[0].wait_recv()
    layer(toks, 0, step, w_one, x, pre_one, h_one)
    relay(0, 6)
    relay(3, 6)
    relay(1, 12)
    relay(2, 6)
    relay(0, 1, 5, 3, 7)
    relay(3, 1, 5, 3, 7)
    layer(toks, 0, step, w_one, other, pre_one, h_one)
    relay(1, 6)
    relay(2, 10, 12)
    tok_copies[1].wait_recv()
    layer(toks, step, half - step, w_one, x, pre_one, h_one)
    layer(toks, step, half - step, w_one, other, pre_one, h_one)
    relay(1, 10, 14)
    layer(h_one, 0, half, w_two, x, pre_two, h_two)
    relay(2, 14)
    relay(1, 1, 9, 5, 13, 3, 11, 7, 15)
    layer(h_one, 0, half, w_two, other, pre_two, h_two)
    relay(2, 1, 9, 5, 13, 3, 11, 7, 15)
    tar_copy.wait_recv()
    tgt[:, at(other, vw)] = tar_all[other].astype(wide).T
    for side in range(2):
        cols = slice(side * vw, (side + 1) * vw)
        error = lax.dot_general(
            h_two[0:half, :], w_head[cols, :], (((1,), (1,)), ((), ())), preferred_element_type=wide
        )
        error = error - tgt[0:half, cols]
        m = masked[:, cols]
        sc = m * error
        scored[:, cols] = sc
        sc_low[0:half, cols] = sc.astype(low)
        esum = jnp.sum(sc * error, axis=0, keepdims=True)
        wsum = jnp.sum(m, axis=0, keepdims=True)
        for n in range(2):
            r = side * 2 + n
            msg[r : r + 1, :] = esum[:, n * TILE : (n + 1) * TILE]
            msg[4 + r : 5 + r, :] = wsum[:, n * TILE : (n + 1) * TILE]

    def share(src, slots, me, peers, base):
        copies = [remote(src, slots.at[me], tsend, trecv, base + n, peer) for n, peer in enumerate(peers)]
        slots[me] = src[...]
        return copies

    first_share = share(msg, near, mine, [near_peer(d) for d in range(1, 8)], 0)

    def scored_cols(side, c):
        return pl.ds(pl.multiple_of(side * vw + c * TILE, TILE), TILE)

    score_copies = [
        remote(sc_low.at[:, scored_cols(n, oc)], sc_par.at[:, pl.ds(n * TILE, TILE)], dsend, drecv, n, partner)
        for n in range(2)
    ]
    flips = [flip_to(h_two, t_two, 2), flip_to(h_one, t_one, 3), flip_to(toks, t_tok, 4)]
    make_slope(pre_two)
    for copy in first_share:
        copy.wait_recv()
    mid[...] = jnp.sum(near[...], axis=0)
    second_share = share(mid, far, high, [far_peer(d) for d in range(1, 4)], 7)

    mark_bits = {"z": zn, "y": yy}

    def goal(way):
        return across if way == "x" else (flipped(s, BITS[way]), x)

    def produce(g, h, trans, own_cols, par_cols):
        first = PLAN[g, h][0]
        both_cols = jnp.concatenate([own_cols, par_cols], axis=0)
        ref, store = fars[g, h][0], nears[g, h][0]

        def product(blocks):
            sides = [
                jnp.concatenate(
                    [trans[k, pl.ds(pl.multiple_of(b * TILE + h * hr, hr), hr), :] for b in blocks], axis=0
                )
                for k in range(2)
            ]
            return jnp.dot(jnp.concatenate(sides, axis=1), both_cols, preferred_element_type=wide)

        def blocks_of(v):
            return [i * 4 + (j * 2 + v if first == "y" else v * 2 + j) for i in range(2) for j in range(2)]

        if first == "x":
            out = product(list(range(8)))
            ref[...] = jnp.where(x == 0, out[:, TILE:], out[:, :TILE]).astype(low).reshape(ref.shape)
            store[...] = jnp.where(x == 0, out[:, :TILE], out[:, TILE:]).reshape(ref.shape)
        else:
            value = mark_bits[first]
            out = product(blocks_of(1 - value) + blocks_of(value))
            ref[...] = out[: 4 * hr].astype(low).reshape(ref.shape)
        copy = remote(ref, arrs[g, h][0], rsend, rrecv, 9 * g + 3 * h, goal(first))
        if first != "x":
            store[...] = out[4 * hr :].reshape(ref.shape)
        return copy

    def advance(g, h, n, copy):
        copy.wait_recv()
        order = PLAN[g, h]
        way = order[n]
        left = [d for d in "fzy" if d not in order[:n]]
        ref, came = nears[g, h][n - 1], arrs[g, h][n - 1]
        if way == "x":
            lead = (slice(None),) * (len(left) + 1)
            away, here = lead + (at(other, TILE),), lead + (at(x, TILE),)
        else:
            lead = (slice(None),) * left.index(way)
            away, here = lead + (1 - mark_bits[way],), lead + (mark_bits[way],)
        fars[g, h][n][...] = (ref[away] + came[away].astype(wide)).astype(low)
        copy = remote(fars[g, h][n], arrs[g, h][n], rsend, rrecv, 9 * g + 3 * h + n, goal(way))
        nears[g, h][n][...] = ref[here] + came[here].astype(wide)
        return copy

    def advance_last(g, before):
        for h in range(2):
            before[h].wait_recv()
            finals[g, h] = (nears2[g, h, 1 - zf] + arrs2[g, h, 1 - zf].astype(wide)).astype(low)
        up = (flipped(s, 3), x)
        copies = [
            remote(finals.at[g, core], arrs4.at[g], rsend, rrecv, 9 * g + 6, up),
            remote(finals.at[g, oc], arrs5.at[g], rsend, rrecv, 9 * g + 7, diagonal),
        ]
        for h in range(2):
            nears2[g, h, zf] = nears2[g, h, zf] + arrs2[g, h, zf].astype(wide)
        copies.append(remote(nears2.at[g, oc, zf], arrs3.at[g], rsend, rrecv, 9 * g + 8, partner))
        return copies

    def finish(g, copies, out, base):
        for copy in copies:
            copy.wait_recv()
        kept = nears2[g, core, zf] + arrs4[g].astype(wide)
        came = arrs3[g] + arrs5[g].astype(wide)
        span = out.shape[1] // 2
        out[pl.ds(0, hr), pl.ds(pl.multiple_of(core * span + base, TILE), TILE)] = kept
        out[pl.ds(0, hr), pl.ds(pl.multiple_of(oc * span + base, TILE), TILE)] = came

    for copy in score_copies:
        copy.wait_recv()
    flips[0].wait_recv()
    state = {}
    own = jnp.concatenate([sc_low[:, scored_cols(n, core)] for n in range(2)], axis=1)
    for h in range(2):
        state[0, h] = produce(0, h, t_two, own, sc_par[...])
    make_slope(pre_one)
    for copy in second_share:
        copy.wait_recv()
    sums = jnp.sum(far[...], axis=0)
    tl = lax.broadcasted_iota(jnp.int32, (8, TILE), 1)
    sums = sums + jnp.where(tl % 2 == 0, pltpu.roll(sums, TILE - 1, 1), pltpu.roll(sums, 1, 1))
    sums = sums + jnp.where(tl % 4 < 2, pltpu.roll(sums, TILE - 2, 1), pltpu.roll(sums, 2, 1))
    kinds = 2 * rows // PP
    line = lax.broadcasted_iota(jnp.int32, (4, TILE), 0)
    tl = lax.broadcasted_iota(jnp.int32, (4, TILE), 1)
    ok = (line % 2) * TILE + tl < rows
    weight_sum = jnp.where(ok, sums[4:8, :], 1.0)
    root = jnp.sqrt(jnp.where(ok, sums[0:4, :], 0.0) / weight_sum + 1e-06)
    roots = jnp.where(ok & (tl % PP == 0), root, 0.0)
    loss = jnp.sum(jnp.sum(roots, axis=0, keepdims=True), axis=1, keepdims=True) / kinds
    o_loss[...] = jnp.broadcast_to(loss, o_loss.shape)
    coef = jnp.where(ok, scale[0] / (kinds * root * weight_sum), 0.0)
    coef = jnp.concatenate([coef[n : n + 1, :] for n in range(4)], axis=1)
    gp_low[...] = (coef * scored[...]).astype(low)

    def grad_tiles(made, send_to, base, make):
        for n in range(dim // vw):
            tile = pl.ds(n * vw, vw)
            made[0:half, tile] = make(tile)
        return [
            remote(
                made.at[:, pl.ds(pl.multiple_of(side * width + oc * vw, vw), vw)],
                send_to.at[:, pl.ds(side * vw, vw)],
                dsend, drecv, base + side, partner,
            )
            for side in range(2)
        ]

    def make_two(tile):
        b = jnp.dot(gp_low[...], w_head[:, tile], preferred_element_type=wide)
        return (b * pre_two[:, tile]).astype(low)

    two_copies = grad_tiles(g_two, p_two, 5, make_two)

    def make_one(tile):
        b = lax.dot_general(
            g_two[0:half, :], w_two[tile, :], (((1,), (1,)), ((), ())), preferred_element_type=wide
        )
        return (b * pre_one[:, tile]).astype(low)

    one_copies = grad_tiles(g_one, p_one, 7, make_one)

    def both(made, came, a):
        own_cols = [
            made[:, pl.ds(pl.multiple_of(n * width + core * vw + a * TILE, TILE), TILE)] for n in range(2)
        ]
        par_cols = [came[:, n * vw + a * TILE : n * vw + (a + 1) * TILE] for n in range(2)]
        return jnp.concatenate(own_cols, axis=1), jnp.concatenate(par_cols, axis=1)

    def token_rows(side, first, size, out, base=0):
        for n in range(width // vw):
            b = lax.dot_general(
                g_one[first : first + size, :],
                w_one[pl.ds(pl.multiple_of(side * width + n * vw, vw), vw), :],
                (((1,), (1,)), ((), ())),
                preferred_element_type=wide,
            )
            place_rows = pl.ds(pl.multiple_of(base + first, 16), size)
            out[place_rows, n * vw : (n + 1) * vw] = b.astype(low)

    results = (hb, o_two, o_two, o_one, o_one)
    tails = []
    waited = set()
    for name in STEPS:
        kind, args = name[0], [int(c) for c in name[1:]]
        if kind == "C":
            token_rows(other, 0, half, tg_far)
        elif kind == "T":
            piece = half // 4
            first = args[0] * piece
            place_out = o_tok.at[pl.ds(pl.multiple_of(x * half + first, 16), piece), :]
            tails.append(remote(tg_far.at[pl.ds(first, piece), :], place_out, xsend, xrecv, 5 + args[0], across))
        elif kind == "N":
            token_rows(x, 0, half, o_tok, x * half)
        elif kind == "P":
            g, h = args
            which = g > 2
            if which not in waited:
                waited.add(which)
                for copy in (one_copies + [flips[2]]) if which else (two_copies + [flips[1]]):
                    copy.wait_recv()
            sources = both(g_one, p_one, g - 3) if which else both(g_two, p_two, g - 1)
            state[g, h] = produce(g, h, t_tok if which else t_one, *sources)
        elif kind == "A":
            g, h, n = args
            state[g, h] = advance(g, h, n, state[g, h])
        elif kind == "L":
            (g,) = args
            state[g] = advance_last(g, [state[g, 0], state[g, 1]])
        else:
            (g,) = args
            finish(g, state[g], results[g], TILE if g in (2, 4) else 0)
            if g == 0:
                coef_here = jnp.where(x == 0, coef[:, :vw], coef[:, vw:])
                o_head[...] = (hb[...] * coef_here)[:, 0:rows]
    for copy in tails:
        copy.wait_recv()
    for copy in started:
        copy.wait_send()


def fused(scale, kinds, land, tokens, first, second, head, targets):
    count, width = tokens.shape
    dim = first.shape[0]
    rows = head.shape[0]
    half = count // 2
    pad = -(-half // TILE) * TILE
    vw = 2 * TILE
    hr = TILE // 2
    low, wide = jnp.bfloat16, jnp.float32
    shape = jax.ShapeDtypeStruct
    slices = SLICES
    vm = pltpu.VMEM
    scratch = [
        vm((dim, dim), low), vm((dim, dim), low), vm((2 * vw, dim), low), vm((pad, dim), low),
        vm((half, width), low), vm((rows, count), wide), vm((rows, pad), low), vm((2, vw, pad), low),
        vm((TILE, count), wide), vm((half, 2 * vw), wide),
        vm((half, dim), wide), vm((half, dim), wide), vm((pad, dim), low), vm((pad, dim), low),
        vm((2, dim, pad), low), vm((2, dim, pad), low), vm((2, dim, pad), low),
        vm((pad, 2 * vw), wide), vm((half, 2 * vw), wide), vm((pad, 2 * vw), low), vm((pad, vw), low),
        vm((half, 2 * vw), low),
        vm((pad, dim), low), vm((pad, dim), low), vm((pad, width), low), vm((pad, width), low),
        vm((half, width), low), vm((hr, vw), wide),
        vm((8, TILE), wide), vm((8, TILE), wide),
        vm((8, TILE), wide), vm((8, 8, TILE), wide), vm((4, 8, TILE), wide), vm((8, TILE), wide),
        vm((slices, 2, hr, TILE), low), vm((slices, hr, TILE), wide),
        vm((slices, hr, TILE), low), vm((slices, hr, TILE), low),
    ]
    for kind in (low, low, wide):
        for key in sorted(PLAN):
            scratch += [vm(found, kind) for found in stage_shapes(PLAN[key])[:2]]
    scratch += [vm((slices, 2, 2, hr, TILE), kind) for kind in (low, low, wide)]
    sizes = (6, 64, 64, 9, 9, 9, 9, 10, 10, 9 * slices, 9 * slices)
    scratch += [pltpu.SemaphoreType.DMA((n,)) for n in sizes]
    return pl.pallas_call(
        fused_kernel,
        out_shape=(
            vm((8, TILE), wide),
            vm((count, width), low),
            vm((dim // 16, width), wide),
            vm((dim // 16, width), wide),
            vm((hr, rows), wide),
        ),
        in_specs=[pl.BlockSpec(memory_space=pltpu.SMEM), VMEM, VMEM] + [HBM] * 5,
        out_specs=[VMEM] * 5,
        scratch_shapes=scratch,
        compiler_params=params(0, 56),
        name="fused",
    )(scale, kinds, land, tokens, first, second, head, targets)


CHUNKS = 4


def write_kernel(loss, tok, one, two, head, o_loss, o_tok, o_one, o_two, o_head, f_loss, f_tok, went):
    size = tok.shape[0] // CHUNKS
    stores = []

    def store(src, dst):
        copy = pltpu.make_async_copy(src, dst, went.at[len(stores)])
        copy.start()
        stores.append(copy)

    store(one, o_one)
    store(two, o_two)
    store(head, o_head)
    f_loss[...] = loss[0:1, 0:1]
    store(f_loss, o_loss)
    for n in range(CHUNKS):
        span = pl.ds(n * size, size)
        f_tok[span, :] = tok[span, :].astype(jnp.float32)
        store(f_tok.at[span, :], o_tok.at[span, :])
    for copy in stores:
        copy.wait()


def write(*parts):
    wide = jnp.float32
    shapes = [(1, 1)] + [p.shape for p in parts[1:]]
    vm = pltpu.VMEM
    return pl.pallas_call(
        write_kernel,
        out_shape=tuple(jax.ShapeDtypeStruct(a, wide) for a in shapes),
        in_specs=[VMEM] * 5,
        out_specs=[ANY] * 5,
        scratch_shapes=[vm((1, 1), wide), vm(parts[1].shape, wide), pltpu.SemaphoreType.DMA((CHUNKS + 4,))],
        compiler_params=pltpu.CompilerParams(vmem_limit_bytes=16 * 2**20),
        name="write",
    )(*parts)


def per_device(
    tokens, first_weight, second_weight, head_weight, targets, land_mask, variable_kind, loss_scale
):
    parts = fused(
        loss_scale.reshape(1), variable_kind.reshape(1, -1), land_mask,
        tokens, first_weight, second_weight, head_weight, targets,
    )
    loss, token_grad, first_grad, second_grad, head_grad = write(*parts)
    return (loss.reshape(()), token_grad, first_grad, second_grad, head_grad.T)


def column_folder(weights, piece):
    return lax.dot_general(
        piece, weights, (((1,), (1,)), ((), ())), preferred_element_type=jnp.float32
    )


def row_folder(weights, piece):
    return lax.dot_general(
        piece, weights, (((0,), (0,)), ((), ())), preferred_element_type=jnp.float32
    )


def per_device_wide(
    tokens, first_weight, second_weight, head_weight, targets, land_mask, variable_kind, loss_scale
):
    count = tokens.shape[0]
    width = first_weight.shape[1]
    kinds = head_weight.shape[0] // PP
    rows_first, rows_second = (
        lax.all_to_all(first_weight, "tensor", split_axis=0, concat_axis=1, tiled=True),
        lax.all_to_all(second_weight, "tensor", split_axis=0, concat_axis=1, tiled=True),
    )
    head_cols = lax.all_to_all(head_weight, "tensor", split_axis=1, concat_axis=0, tiled=True)
    position = lax.axis_index("space") * count + jnp.arange(count, dtype=jnp.int32)
    cell = jnp.arange(PP, dtype=jnp.int32)
    lat_row = 2 * (position // LONP)[None, :] + (cell // 2)[:, None]
    nlat = 2 * PROW_DEV * lax.axis_size("space")
    cell_weight = jnp.cos(math.pi / 2.0 * (lat_row.astype(jnp.float32) + 0.5) / nlat)
    land = land_mask.astype(jnp.float32)
    kind = variable_kind[:, None, None]
    valid = jnp.where(kind == 0, 1.0, jnp.where(kind == 1, land[None], 1.0 - land[None]))
    masked = cell_weight[None] * valid
    local_weight = jnp.sum(masked, axis=(1, 2))
    weight_sum = lax.psum(local_weight, "space")
    full_in = lax.all_gather(tokens, "tensor", axis=1, tiled=True)
    pre_one = jnp.dot(full_in, first_weight, preferred_element_type=jnp.float32)
    hidden_one = jax.nn.gelu(pre_one, approximate=False).astype(jnp.bfloat16)
    full_one = lax.all_gather(hidden_one, "tensor", axis=1, tiled=True)
    pre_two = jnp.dot(full_one, second_weight, preferred_element_type=jnp.float32)
    hidden_two = jax.nn.gelu(pre_two, approximate=False).astype(jnp.bfloat16)
    full_two = lax.all_gather(hidden_two, "tensor", axis=1, tiled=True)
    predicted = lax.dot_general(
        head_weight, full_two, (((1,), (1,)), ((), ())), preferred_element_type=jnp.float32
    )
    error = predicted.reshape(kinds, PP, count) - targets.reshape(kinds, PP, count)
    local_error = jnp.sum(masked * error * error, axis=(1, 2))
    error_sum = lax.psum(local_error, "space")
    root = jnp.sqrt(error_sum / weight_sum + 1e-06)
    loss = lax.psum(jnp.sum(root), "tensor") / (kinds * lax.axis_size("tensor"))
    coef = loss_scale / (kinds * lax.axis_size("tensor") * root * weight_sum)
    grad_pred = (
        (coef[:, None, None] * masked * error).reshape(kinds * PP, count).astype(jnp.bfloat16)
    )
    back_two = row_folder(head_cols, lax.all_gather(grad_pred, "tensor", axis=0, tiled=True))
    head_term = jnp.dot(grad_pred, full_two, preferred_element_type=jnp.float32)
    head_grad = lax.psum_scatter(head_term, "space", scatter_dimension=1, tiled=True)
    grad_two = (back_two * slope(pre_two)).astype(jnp.bfloat16)
    back_one = column_folder(rows_second, lax.all_gather(grad_two, "tensor", axis=1, tiled=True))
    grad_one = (back_one * slope(pre_one)).astype(jnp.bfloat16)
    joined = lax.psum_scatter(
        jnp.concatenate(
            [
                lax.dot_general(
                    full_one, grad_two, (((0,), (0,)), ((), ())), preferred_element_type=jnp.float32
                ),
                lax.dot_general(
                    full_in, grad_one, (((0,), (0,)), ((), ())), preferred_element_type=jnp.float32
                ),
            ],
            axis=1,
        ),
        "space",
        scatter_dimension=0,
        tiled=True,
    )
    second_grad = joined[:, :width]
    first_grad = joined[:, width:]
    token_grad = column_folder(rows_first, lax.all_gather(grad_one, "tensor", axis=1, tiled=True))
    return (loss, token_grad, first_grad, second_grad, head_grad)


def solution(mesh):
    size = mesh.shape["space"]
    paired = mesh.shape["tensor"] == 2 and size == 16
    return jax.shard_map(
        per_device if paired else per_device_wide,
        mesh=mesh,
        in_specs=(
            P("space", "tensor"),
            P(None, "tensor"),
            P(None, "tensor"),
            P("tensor", None),
            P("tensor", "space"),
            P(None, "space"),
            P("tensor"),
            P(),
        ),
        out_specs=(
            P(),
            P("space", "tensor"),
            P("space", "tensor"),
            P("space", "tensor"),
            P("tensor", "space"),
        ),
        check_vma=False,
    )
```
